8 devices in a mesh: dp: 2 (over y, z), tp: 4 (over x, core).
Axes of the slice: x: 2, y: 2, z: 1, core: 2. Of those that a mesh axis runs over, the one named last changes fastest.
Arguments:
- x: bfloat16 [256, 4096], P('dp'), parts along dimension 0
- w_gate: bfloat16 [4096, 16384], P(None, 'tp')
- w_up: bfloat16 [4096, 16384], P(None, 'tp')
- w_down: bfloat16 [16384, 4096], P('tp')
Outputs:
- output: bfloat16 [256, 4096], P('dp'), parts along dimension 0
There are 2 independent parts. The reference program is written for one: setup_inputs(seed, part) draws one part's arguments, and reference() takes and returns one part's arrays. A program takes and returns all parts, laid end to end along the dimension named above; an argument that names none is the same for every part.
All inputs are finite; a program needn't handle non-finite values.
Results may differ from the reference program's by a relative error of at most 0.016.
Values are sent between devices in bfloat16 or wider.
A program may use at most 2 GiB of HBM per device.

```python
import jax
import jax.numpy as jnp

ROWS = 128
D = 4096
FF = 16384


def setup_inputs(seed: int = 0, part: int = 0) -> dict:
    kx, kg, ku, kd = jax.random.split(jax.random.key(seed), 4)
    drawn = {
        "x": jax.random.normal(jax.random.fold_in(kx, part), (ROWS, D), jnp.float32),
        "w_gate": jax.random.normal(kg, (D, FF), jnp.float32) * D**-0.5,
        "w_up": jax.random.normal(ku, (D, FF), jnp.float32) * D**-0.5,
        "w_down": jax.random.normal(kd, (FF, D), jnp.float32) * FF**-0.5,
    }
    return {k: v.astype(jnp.bfloat16) for k, v in drawn.items()}


def reference(x, w_gate, w_up, w_down):
    gate = jnp.dot(x, w_gate, preferred_element_type=jnp.float32)
    up = jnp.dot(x, w_up, preferred_element_type=jnp.float32)
    hidden = (jax.nn.silu(gate) * up).astype(jnp.bfloat16)
    return jnp.dot(hidden, w_down, preferred_element_type=jnp.float32).astype(jnp.bfloat16)
```

```python
import functools

import jax
import jax.numpy as jnp
from jax import lax
from jax.experimental import pallas as pl
from jax.experimental.pallas import tpu as pltpu
from jax.sharding import PartitionSpec as P

MESH = pl.DeviceIdType.MESH
ROWS = 128
HALF = ROWS // 2
D = 4096
F = 4096
BN = 256
SLOTS = 8
NG = F // BN
DB = 2 * BN
ND = D // DB
LAG_X = 1
LAG_Y = 4


def kernel(x_hbm, wg_hbm, wu_hbm, wd_hbm, y_ref,
           xv, h, w, tb, tf, rb, ub, xr, x_sem, w_sem,
           d_send, d_recv, u_send, u_recv, g_send, g_recv):
    tp = lax.axis_index("tp")
    core = lax.rem(tp, 2)
    chip = tp // 2
    partner = {"tp": 2 * chip + (1 - core)}
    across = {"tp": 2 * (1 - chip) + core}
    mine = pl.ds(pl.multiple_of(core * HALF, HALF), HALF)
    theirs = pl.ds(pl.multiple_of((1 - core) * HALF, HALF), HALF)

    def gu_copies(i, s):
        cols = pl.ds(pl.multiple_of(i * BN, BN), BN)
        return (pltpu.make_async_copy(wg_hbm.at[:, cols], w.at[s, 0], w_sem.at[s, 0]),
                pltpu.make_async_copy(wu_hbm.at[:, cols], w.at[s, 1], w_sem.at[s, 1]))

    def d_copies(j, s):
        return tuple(
            pltpu.make_async_copy(
                wd_hbm.at[:, pl.ds(pl.multiple_of(j * DB + q * BN, BN), BN)], w.at[s, q], w_sem.at[s, q])
            for q in range(2))

    x_copy = pltpu.make_async_copy(x_hbm, xv, x_sem)
    x_copy.start()
    for s in range(SLOTS):
        for c in gu_copies(s, s):
            c.start()

    barrier = pltpu.get_barrier_semaphore()
    for peer in (partner, across):
        pl.semaphore_signal(barrier, inc=1, device_id=peer, device_id_type=MESH)
    pl.semaphore_wait(barrier, 2)

    x_copy.wait()

    def gu_step(i, carry):
        s = lax.rem(i, SLOTS)
        for c in gu_copies(i, s):
            c.wait()
        gate = jnp.dot(xv[...], w[s, 0], preferred_element_type=jnp.float32)
        up = jnp.dot(xv[...], w[s, 1], preferred_element_type=jnp.float32)
        h[:, pl.ds(pl.multiple_of(i * BN, BN), BN)] = (jax.nn.silu(gate) * up).astype(jnp.bfloat16)
        nxt = i + SLOTS

        @pl.when(nxt < NG)
        def _():
            for c in gu_copies(nxt, s):
                c.start()

        @pl.when(nxt >= NG)
        def _():
            for c in d_copies(nxt - NG, s):
                c.start()

        return carry

    lax.fori_loop(0, NG, gu_step, 0)

    def d_core(j):
        return pltpu.make_async_remote_copy(
            tb.at[j, theirs], rb.at[j], d_send.at[j], d_recv.at[j], device_id=partner, device_id_type=MESH)

    def d_across(j):
        return pltpu.make_async_remote_copy(
            ub.at[j], xr.at[j], u_send.at[j], u_recv.at[j], device_id=across, device_id_type=MESH)

    def d_gather(j):
        part = y_ref.at[mine, pl.ds(j * DB, DB)]
        return pltpu.make_async_remote_copy(
            part, part, g_send.at[j], g_recv.at[j], device_id=partner, device_id_type=MESH)

    def reduce_and_cross(j):
        d_core(j).wait_recv()
        ub[j] = (tf[j % 2, mine, :] + rb[j].astype(jnp.float32)).astype(jnp.bfloat16)
        d_across(j).start()

    def finish(j):
        d_across(j).wait_recv()
        y_ref[mine, pl.ds(j * DB, DB)] = (
            ub[j].astype(jnp.float32) + xr[j].astype(jnp.float32)).astype(jnp.bfloat16)
        d_gather(j).start()

    for j in range(ND):
        s = (NG + j) % SLOTS
        for q, c in enumerate(d_copies(j, s)):
            c.wait()
            term = jnp.dot(h[...], w[s, q], preferred_element_type=jnp.float32)
            tf[j % 2, :, pl.ds(q * BN, BN)] = term
            tb[j, :, pl.ds(q * BN, BN)] = term.astype(jnp.bfloat16)
        d_core(j).start()
        if j >= LAG_X:
            reduce_and_cross(j - LAG_X)
        if j >= LAG_Y:
            finish(j - LAG_Y)
    for j in range(ND - LAG_X, ND):
        reduce_and_cross(j)
    for j in range(ND - LAG_Y, ND):
        finish(j)
    for j in range(ND):
        d_core(j).wait_send()
        d_across(j).wait_send()
        d_gather(j).wait_send()
        d_gather(j).wait_recv()


def mlp(x, w_gate, w_up, w_down):
    bf = jnp.bfloat16
    dma = pltpu.SemaphoreType.DMA
    return pl.pallas_call(
        kernel,
        name="mlp",
        out_shape=jax.ShapeDtypeStruct((ROWS, D), bf),
        in_specs=[pl.BlockSpec(memory_space=pl.ANY)] * 4,
        out_specs=pl.BlockSpec(memory_space=pltpu.VMEM),
        scratch_shapes=[
            pltpu.VMEM((ROWS, D), bf),
            pltpu.VMEM((ROWS, F), bf),
            pltpu.VMEM((SLOTS, 2, D, BN), bf),
            pltpu.VMEM((ND, ROWS, DB), bf),
            pltpu.VMEM((2, ROWS, DB), jnp.float32),
            pltpu.VMEM((ND, HALF, DB), bf),
            pltpu.VMEM((ND, HALF, DB), bf),
            pltpu.VMEM((ND, HALF, DB), bf),
            dma, dma((SLOTS, 2)),
            dma((ND,)), dma((ND,)), dma((ND,)), dma((ND,)), dma((ND,)), dma((ND,)),
        ],
        compiler_params=pltpu.CompilerParams(
            collective_id=0, has_side_effects=True, vmem_limit_bytes=60 * 1024 * 1024),
    )(x, w_gate, w_up, w_down)


def solution(mesh):
    return jax.shard_map(
        mlp,
        mesh=mesh,
        in_specs=(P("dp", None), P(None, "tp"), P(None, "tp"), P("tp", None)),
        out_specs=P("dp", None),
        check_vma=False,
    )
```

```python
import functools

import jax
import jax.numpy as jnp
from jax import lax
from jax.experimental import pallas as pl
from jax.experimental.pallas import tpu as pltpu
from jax.sharding import PartitionSpec as P

MESH = pl.DeviceIdType.MESH
F32 = jnp.float32
BF16 = jnp.bfloat16
ROWS = 128
HALF = ROWS // 2
D = 4096
F = 4096
FH = F // 2
KC = 512
NK = D // KC
XC = 256
NR = 6
NC = 4
NB = 256
DB = 512
ND = D // DB
LAG = 3


def kernel(x_hbm, wg_hbm, wu_hbm, wd_hbm, y_ref,
           xs, xo, wg, wu, wd, acc_s, acc_o, h_s, h_o,
           tb_o, rb_o, uy, yr, tb_s, rb_s, ux, xr,
           x_sem, g_sem, u_sem, w_sem,
           yx_send, yx_recv, xx_send, xx_recv, dx_send, dx_recv,
           do_send, do_recv, uy_send, uy_recv, ds_send, ds_recv,
           ux_send, ux_recv, gy_send, gy_recv):
    grp = lax.axis_index("dp")
    tp = lax.axis_index("tp")
    core = lax.rem(tp, 2)
    chip = tp // 2
    partner = {"tp": 2 * chip + (1 - core)}
    xpeer = {"tp": 2 * (1 - chip) + core}
    ypeer = {"dp": 1 - grp}
    mine = pl.ds(pl.multiple_of(core * HALF, HALF), HALF)
    theirs = pl.ds(pl.multiple_of((1 - core) * HALF, HALF), HALF)
    units = pl.ds(pl.multiple_of(grp * FH, FH), FH)

    x_copy = pltpu.make_async_copy(x_hbm, xs, x_sem)

    def w_copies(k):
        rows = pl.ds(k * KC, KC)
        return (pltpu.make_async_copy(wg_hbm.at[rows, units], wg.at[k], g_sem.at[k]),
                pltpu.make_async_copy(wu_hbm.at[rows, units], wu.at[k], u_sem.at[k]))

    def wd_copy(j):
        return pltpu.make_async_copy(wd_hbm.at[units, pl.ds(j * DB, DB)], wd.at[j], w_sem.at[j])

    def push(src, dst, send, recv, peer):
        return pltpu.make_async_remote_copy(src, dst, send, recv, device_id=peer, device_id_type=MESH)

    def relay_k(i, c):
        return 2 * (i // 2) + c

    def relay_cols(i, c):
        return pl.ds(pl.multiple_of(relay_k(i, c) * KC + (i % 2) * XC, XC), XC)

    def y_cols(i):
        if i < NR:
            return relay_cols(i, chip)
        return pl.ds(2 * NR * XC + (i - NR) * XC, XC)

    def y_x(i):
        c = y_cols(i)
        return push(xs.at[mine, c], xo.at[mine, c], yx_send.at[i], yx_recv.at[i], ypeer)

    def x_x(i, c):
        c = relay_cols(i, c)
        return push(xo.at[mine, c], xo.at[mine, c], xx_send.at[i], xx_recv.at[i], xpeer)

    def d_x(i):
        c = y_cols(i) if i < NR + NC else relay_cols(i - NR - NC, 1 - chip)
        return push(xo.at[mine, c], xo.at[mine, c], dx_send.at[i], dx_recv.at[i], partner)

    def on_y(i):
        y_x(i).wait_recv()
        if i < NR:
            x_x(i, chip).start()
        d_x(i).start()

    def on_x(i):
        x_x(i, 1 - chip).wait_recv()
        d_x(NR + NC + i).start()

    x_copy.start()
    for k in range(NK):
        for c in w_copies(k):
            c.start()
    for j in range(ND):
        wd_copy(j).start()

    barrier = pltpu.get_barrier_semaphore()
    for peer in (partner, xpeer, ypeer):
        pl.semaphore_signal(barrier, inc=1, device_id=peer, device_id_type=MESH)
    pl.semaphore_wait(barrier, 3)

    x_copy.wait()
    for i in range(NR + NC):
        y_x(i).start()

    def gate_up(xref, acc, k, first=False, h=None):
        cols = pl.ds(k * KC if isinstance(k, int) else pl.multiple_of(k * KC, KC), KC)
        for n in range(0, FH, NB):
            nn = pl.ds(n, NB)
            g = jnp.dot(xref[:, cols], wg[k, :, nn], preferred_element_type=F32)
            u = jnp.dot(xref[:, cols], wu[k, :, nn], preferred_element_type=F32)
            if not first:
                g = acc[0, :, nn] + g
                u = acc[1, :, nn] + u
            if h is None:
                acc[0, :, nn] = g
                acc[1, :, nn] = u
            else:
                h[:, nn] = (jax.nn.silu(g) * u).astype(BF16)

    def own(k):
        for c in w_copies(k):
            c.wait()
        gate_up(xs, acc_s, k, first=k == 0, h=h_s if k == NK - 1 else None)

    def oth_y(r, first=False):
        for i in (2 * r, 2 * r + 1):
            d_x(i).wait_recv()
        gate_up(xo, acc_o, relay_k(2 * r, chip), first=first)

    def oth_x(r):
        for i in (2 * r, 2 * r + 1):
            d_x(NR + NC + i).wait_recv()
        gate_up(xo, acc_o, relay_k(2 * r, 1 - chip))

    def oth_c(r, last=False):
        for i in (2 * r, 2 * r + 1):
            d_x(NR + i).wait_recv()
        gate_up(xo, acc_o, NR + r, h=h_o if last else None)

    def wait_w(k):
        for c in w_copies(k):
            c.wait()

    own(0)
    own(1)
    on_y(0)
    own(2)
    on_y(1)
    on_y(2)
    own(3)
    on_y(3)
    oth_y(0, first=True)
    on_y(4)
    on_x(0)
    own(4)
    on_y(5)
    on_x(1)
    oth_y(1)
    on_y(6)
    on_x(2)
    own(5)
    on_y(7)
    oth_y(2)
    on_x(3)
    on_y(8)
    oth_x(0)
    on_x(4)
    on_y(9)
    on_x(5)
    wait_w(6)
    oth_c(0)
    oth_x(1)
    oth_x(2)
    wait_w(7)
    oth_c(1, last=True)

    def cols_of(j):
        return (j * DB) // FH, pl.ds((j * DB) % FH, DB)

    def term(h, acc, tb, j):
        q, cc = cols_of(j)
        acc[q, :, cc] = jnp.dot(h[...], wd[j], preferred_element_type=F32)
        tb[j] = acc[q, theirs, cc].astype(BF16)

    def core_o(j):
        return push(tb_o.at[j], rb_o.at[j], do_send.at[j], do_recv.at[j], partner)

    def core_s(j):
        return push(tb_s.at[j], rb_s.at[j], ds_send.at[j], ds_recv.at[j], partner)

    def over_y(j):
        return push(uy.at[j], yr.at[j], uy_send.at[j], uy_recv.at[j], ypeer)

    def over_x(j):
        return push(ux.at[j], xr.at[j], ux_send.at[j], ux_recv.at[j], xpeer)

    def gather(j):
        part = y_ref.at[mine, pl.ds(j * DB, DB)]
        return push(part, part, gy_send.at[j], gy_recv.at[j], partner)

    def send_y(j):
        q, cc = cols_of(j)
        core_o(j).wait_recv()
        uy[j] = (acc_o[q, mine, cc] + rb_o[j].astype(F32)).astype(BF16)
        over_y(j).start()

    def send_x(j):
        q, cc = cols_of(j)
        core_s(j).wait_recv()
        over_y(j).wait_recv()
        ux[j] = (acc_s[q, mine, cc] + rb_s[j].astype(F32) + yr[j].astype(F32)).astype(BF16)
        over_x(j).start()

    def finish(j):
        over_x(j).wait_recv()
        y_ref[mine, pl.ds(j * DB, DB)] = (ux[j].astype(F32) + xr[j].astype(F32)).astype(BF16)
        gather(j).start()

    def cross(j):
        send_x(j)
        if j >= LAG:
            finish(j - LAG)

    for j in range(ND):
        wd_copy(j).wait()
        term(h_o, acc_o, tb_o, j)
        core_o(j).start()
        if j >= 2:
            send_y(j - 2)
    gate_up(xs, acc_s, 6)
    send_y(ND - 2)
    send_y(ND - 1)
    gate_up(xs, acc_s, 7, h=h_s)
    for j in range(ND):
        term(h_s, acc_s, tb_s, j)
        core_s(j).start()
        if j >= LAG:
            cross(j - LAG)
    for j in range(ND - LAG, ND):
        cross(j)
    for j in range(ND - LAG, ND):
        finish(j)
    for i in range(NR + NC):
        y_x(i).wait_send()
        d_x(i).wait_send()
    for i in range(NR):
        x_x(i, chip).wait_send()
        d_x(NR + NC + i).wait_send()
    for j in range(ND):
        core_o(j).wait_send()
        core_s(j).wait_send()
        over_y(j).wait_send()
        over_x(j).wait_send()
        gather(j).wait_send()
        gather(j).wait_recv()


def mlp(x, w_gate, w_up, w_down):
    dma = pltpu.SemaphoreType.DMA
    part = pltpu.VMEM((ND, HALF, DB), BF16)
    return pl.pallas_call(
        kernel,
        name="mlp",
        out_shape=jax.ShapeDtypeStruct((ROWS, D), BF16),
        in_specs=[pl.BlockSpec(memory_space=pl.ANY)] * 4,
        out_specs=pl.BlockSpec(memory_space=pltpu.VMEM),
        scratch_shapes=[
            pltpu.VMEM((ROWS, D), BF16),
            pltpu.VMEM((ROWS, D), BF16),
            pltpu.VMEM((NK, KC, FH), BF16),
            pltpu.VMEM((NK, KC, FH), BF16),
            pltpu.VMEM((ND, FH, DB), BF16),
            pltpu.VMEM((2, ROWS, FH), F32),
            pltpu.VMEM((2, ROWS, FH), F32),
            pltpu.VMEM((ROWS, FH), BF16),
            pltpu.VMEM((ROWS, FH), BF16),
            part, part, part, part, part, part, part, part,
            dma, dma((NK,)), dma((NK,)), dma((ND,)),
            dma((NR + NC,)), dma((NR + NC,)), dma((NR,)), dma((NR,)),
            dma((2 * NR + NC,)), dma((2 * NR + NC,)),
            dma((ND,)), dma((ND,)), dma((ND,)), dma((ND,)), dma((ND,)), dma((ND,)),
            dma((ND,)), dma((ND,)), dma((ND,)), dma((ND,)),
        ],
        compiler_params=pltpu.CompilerParams(
            collective_id=0, has_side_effects=True, vmem_limit_bytes=67043328),
    )(x, w_gate, w_up, w_down)


def solution(mesh):
    return jax.shard_map(
        mlp,
        mesh=mesh,
        in_specs=(P("dp", None), P(None, "tp"), P(None, "tp"), P("tp", None)),
        out_specs=P("dp", None),
        check_vma=False,
    )
```

```python
import functools

import jax
import jax.numpy as jnp
from jax import lax
from jax.experimental import pallas as pl
from jax.experimental.pallas import tpu as pltpu
from jax.sharding import PartitionSpec as P

MESH = pl.DeviceIdType.MESH
F32 = jnp.float32
BF16 = jnp.bfloat16
ROWS = 128
HALF = ROWS // 2
D = 4096
F = 4096
FH = F // 2
KC = 512
NK = D // KC
XC = 256
NR = 6
NC = 4
NB = 256
DB = 512
ND = D // DB
LAG = 3
DEPTH = 2


def kernel(x_hbm, wg_hbm, wu_hbm, wd_hbm, y_ref,
           xs, xo, wg, wu, wd, acc_s, acc_o, h_s, h_o,
           tb_o, rb_o, uy, yr, tb_s, rb_s, ux, xr,
           x_sem, g_sem, u_sem, w_sem,
           yx_send, yx_recv, xx_send, xx_recv, dx_send, dx_recv,
           do_send, do_recv, uy_send, uy_recv, ds_send, ds_recv,
           ux_send, ux_recv, gy_send, gy_recv):
    grp = lax.axis_index("dp")
    tp = lax.axis_index("tp")
    core = lax.rem(tp, 2)
    chip = tp // 2
    partner = {"tp": 2 * chip + (1 - core)}
    xpeer = {"tp": 2 * (1 - chip) + core}
    ypeer = {"dp": 1 - grp}
    mine = pl.ds(pl.multiple_of(core * HALF, HALF), HALF)
    theirs = pl.ds(pl.multiple_of((1 - core) * HALF, HALF), HALF)
    units = pl.ds(pl.multiple_of(grp * FH, FH), FH)

    x_copy = pltpu.make_async_copy(x_hbm, xs, x_sem)

    def w_copies(k):
        rows = pl.ds(k * KC, KC)
        return (pltpu.make_async_copy(wg_hbm.at[rows, units], wg.at[k], g_sem.at[k]),
                pltpu.make_async_copy(wu_hbm.at[rows, units], wu.at[k], u_sem.at[k]))

    def wd_copy(j):
        return pltpu.make_async_copy(wd_hbm.at[units, pl.ds(j * DB, DB)], wd.at[j], w_sem.at[j])

    def push(src, dst, send, recv, peer):
        return pltpu.make_async_remote_copy(src, dst, send, recv, device_id=peer, device_id_type=MESH)

    def relay_k(i, c):
        return 2 * (i // 2) + c

    def relay_cols(i, c):
        return pl.ds(pl.multiple_of(relay_k(i, c) * KC + (i % 2) * XC, XC), XC)

    def y_cols(i):
        if i < NR:
            return relay_cols(i, chip)
        return pl.ds(2 * NR * XC + (i - NR) * XC, XC)

    def y_x(i):
        c = y_cols(i)
        return push(xs.at[mine, c], xo.at[mine, c], yx_send.at[i], yx_recv.at[i], ypeer)

    def x_x(i, c):
        c = relay_cols(i, c)
        return push(xo.at[mine, c], xo.at[mine, c], xx_send.at[i], xx_recv.at[i], xpeer)

    def d_x(i):
        c = y_cols(i) if i < NR + NC else relay_cols(i - NR - NC, 1 - chip)
        return push(xo.at[mine, c], xo.at[mine, c], dx_send.at[i], dx_recv.at[i], partner)

    def on_y(i):
        y_x(i).wait_recv()
        if i < NR:
            x_x(i, chip).start()
        d_x(i).start()

    def on_x(i):
        x_x(i, 1 - chip).wait_recv()
        d_x(NR + NC + i).start()

    x_copy.start()
    def more(n):
        for _ in range(n):
            if queue:
                queue.pop(0).start()

    queue = [c for k in range(NK) for c in w_copies(k)] + [wd_copy(j) for j in range(ND)]
    more(2 * DEPTH)

    barrier = pltpu.get_barrier_semaphore()
    for peer in (partner, xpeer, ypeer):
        pl.semaphore_signal(barrier, inc=1, device_id=peer, device_id_type=MESH)
    pl.semaphore_wait(barrier, 3)

    x_copy.wait()
    for i in range(NR + NC):
        y_x(i).start()

    def gate_up(xref, acc, k, first=False, h=None):
        cols = pl.ds(k * KC if isinstance(k, int) else pl.multiple_of(k * KC, KC), KC)
        for n in range(0, FH, NB):
            nn = pl.ds(n, NB)
            g = jnp.dot(xref[:, cols], wg[k, :, nn], preferred_element_type=F32)
            u = jnp.dot(xref[:, cols], wu[k, :, nn], preferred_element_type=F32)
            if not first:
                g = acc[0, :, nn] + g
                u = acc[1, :, nn] + u
            if h is None:
                acc[0, :, nn] = g
                acc[1, :, nn] = u
            else:
                h[:, nn] = (jax.nn.silu(g) * u).astype(BF16)

    def own(k):
        wait_w(k)
        gate_up(xs, acc_s, k, first=k == 0, h=h_s if k == NK - 1 else None)

    def oth_y(r, first=False):
        for i in (2 * r, 2 * r + 1):
            d_x(i).wait_recv()
        gate_up(xo, acc_o, relay_k(2 * r, chip), first=first)

    def oth_x(r):
        for i in (2 * r, 2 * r + 1):
            d_x(NR + NC + i).wait_recv()
        gate_up(xo, acc_o, relay_k(2 * r, 1 - chip))

    def oth_c(r, last=False):
        for i in (2 * r, 2 * r + 1):
            d_x(NR + i).wait_recv()
        gate_up(xo, acc_o, NR + r, h=h_o if last else None)

    def wait_w(k):
        for c in w_copies(k):
            c.wait()
            more(1)

    own(0)
    own(1)
    on_y(0)
    own(2)
    on_y(1)
    on_y(2)
    own(3)
    on_y(3)
    oth_y(0, first=True)
    on_y(4)
    on_x(0)
    own(4)
    on_y(5)
    on_x(1)
    oth_y(1)
    on_y(6)
    on_x(2)
    own(5)
    on_y(7)
    oth_y(2)
    on_x(3)
    on_y(8)
    oth_x(0)
    on_x(4)
    on_y(9)
    on_x(5)
    wait_w(6)
    oth_c(0)
    oth_x(1)
    oth_x(2)
    wait_w(7)
    oth_c(1, last=True)

    def cols_of(j):
        return (j * DB) // FH, pl.ds((j * DB) % FH, DB)

    def term(h, acc, tb, j):
        q, cc = cols_of(j)
        acc[q, :, cc] = jnp.dot(h[...], wd[j], preferred_element_type=F32)
        tb[j] = acc[q, theirs, cc].astype(BF16)

    def core_o(j):
        return push(tb_o.at[j], rb_o.at[j], do_send.at[j], do_recv.at[j], partner)

    def core_s(j):
        return push(tb_s.at[j], rb_s.at[j], ds_send.at[j], ds_recv.at[j], partner)

    def over_y(j):
        return push(uy.at[j], yr.at[j], uy_send.at[j], uy_recv.at[j], ypeer)

    def over_x(j):
        return push(ux.at[j], xr.at[j], ux_send.at[j], ux_recv.at[j], xpeer)

    def gather(j):
        part = y_ref.at[mine, pl.ds(j * DB, DB)]
        return push(part, part, gy_send.at[j], gy_recv.at[j], partner)

    def send_y(j):
        q, cc = cols_of(j)
        core_o(j).wait_recv()
        uy[j] = (acc_o[q, mine, cc] + rb_o[j].astype(F32)).astype(BF16)
        over_y(j).start()

    def send_x(j):
        q, cc = cols_of(j)
        core_s(j).wait_recv()
        over_y(j).wait_recv()
        ux[j] = (acc_s[q, mine, cc] + rb_s[j].astype(F32) + yr[j].astype(F32)).astype(BF16)
        over_x(j).start()

    def finish(j):
        over_x(j).wait_recv()
        y_ref[mine, pl.ds(j * DB, DB)] = (ux[j].astype(F32) + xr[j].astype(F32)).astype(BF16)
        gather(j).start()

    def cross(j):
        send_x(j)
        if j >= LAG:
            finish(j - LAG)

    for j in range(ND):
        wd_copy(j).wait()
        more(1)
        term(h_o, acc_o, tb_o, j)
        core_o(j).start()
        if j >= 2:
            send_y(j - 2)
    gate_up(xs, acc_s, 6)
    send_y(ND - 2)
    send_y(ND - 1)
    gate_up(xs, acc_s, 7, h=h_s)
    for j in range(ND):
        term(h_s, acc_s, tb_s, j)
        core_s(j).start()
        if j >= LAG:
            cross(j - LAG)
    for j in range(ND - LAG, ND):
        cross(j)
    for j in range(ND - LAG, ND):
        finish(j)
    for i in range(NR + NC):
        y_x(i).wait_send()
        d_x(i).wait_send()
    for i in range(NR):
        x_x(i, chip).wait_send()
        d_x(NR + NC + i).wait_send()
    for j in range(ND):
        core_o(j).wait_send()
        core_s(j).wait_send()
        over_y(j).wait_send()
        over_x(j).wait_send()
        gather(j).wait_send()
        gather(j).wait_recv()


def mlp(x, w_gate, w_up, w_down):
    dma = pltpu.SemaphoreType.DMA
    part = pltpu.VMEM((ND, HALF, DB), BF16)
    return pl.pallas_call(
        kernel,
        name="mlp",
        out_shape=jax.ShapeDtypeStruct((ROWS, D), BF16),
        in_specs=[pl.BlockSpec(memory_space=pl.ANY)] * 4,
        out_specs=pl.BlockSpec(memory_space=pltpu.VMEM),
        scratch_shapes=[
            pltpu.VMEM((ROWS, D), BF16),
            pltpu.VMEM((ROWS, D), BF16),
            pltpu.VMEM((NK, KC, FH), BF16),
            pltpu.VMEM((NK, KC, FH), BF16),
            pltpu.VMEM((ND, FH, DB), BF16),
            pltpu.VMEM((2, ROWS, FH), F32),
            pltpu.VMEM((2, ROWS, FH), F32),
            pltpu.VMEM((ROWS, FH), BF16),
            pltpu.VMEM((ROWS, FH), BF16),
            part, part, part, part, part, part, part, part,
            dma, dma((NK,)), dma((NK,)), dma((ND,)),
            dma((NR + NC,)), dma((NR + NC,)), dma((NR,)), dma((NR,)),
            dma((2 * NR + NC,)), dma((2 * NR + NC,)),
            dma((ND,)), dma((ND,)), dma((ND,)), dma((ND,)), dma((ND,)), dma((ND,)),
            dma((ND,)), dma((ND,)), dma((ND,)), dma((ND,)),
        ],
        compiler_params=pltpu.CompilerParams(
            collective_id=0, has_side_effects=True, vmem_limit_bytes=67043328),
    )(x, w_gate, w_up, w_down)


def solution(mesh):
    return jax.shard_map(
        mlp,
        mesh=mesh,
        in_specs=(P("dp", None), P(None, "tp"), P(None, "tp"), P("tp", None)),
        out_specs=P("dp", None),
        check_vma=False,
    )
```

```python
import functools

import jax
import jax.numpy as jnp
from jax import lax
from jax.experimental import pallas as pl
from jax.experimental.pallas import tpu as pltpu
from jax.sharding import PartitionSpec as P

MESH = pl.DeviceIdType.MESH
F32 = jnp.float32
BF16 = jnp.bfloat16
ROWS = 128
HALF = ROWS // 2
D = 4096
F = 4096
FH = F // 2
KC = 512
NK = D // KC
XC = 256
NR = 6
NC = 4
NB = 256
DB = 512
ND = D // DB
LAG = 3
KP = 128
FP = 512


def kernel(x_hbm, wg_hbm, wu_hbm, wd_hbm, y_ref,
           xs, xo, wg, wu, wd, acc_s, acc_o, h_s, h_o,
           tb_o, rb_o, uy, yr, tb_s, rb_s, ux, xr,
           x_sem, g_sem, u_sem, w_sem,
           yx_send, yx_recv, xx_send, xx_recv, dx_send, dx_recv,
           do_send, do_recv, uy_send, uy_recv, ds_send, ds_recv,
           ux_send, ux_recv, gy_send, gy_recv):
    grp = lax.axis_index("dp")
    tp = lax.axis_index("tp")
    core = lax.rem(tp, 2)
    chip = tp // 2
    partner = {"tp": 2 * chip + (1 - core)}
    xpeer = {"tp": 2 * (1 - chip) + core}
    ypeer = {"dp": 1 - grp}
    mine = pl.ds(pl.multiple_of(core * HALF, HALF), HALF)
    theirs = pl.ds(pl.multiple_of((1 - core) * HALF, HALF), HALF)
    units = pl.ds(pl.multiple_of(grp * FH, FH), FH)

    x_copy = pltpu.make_async_copy(x_hbm, xs, x_sem)

    def w_copies(k):
        rows = pl.ds(k * KC, KC)
        return (pltpu.make_async_copy(wg_hbm.at[rows, units], wg.at[k], g_sem.at[k]),
                pltpu.make_async_copy(wu_hbm.at[rows, units], wu.at[k], u_sem.at[k]))

    def w_pieces(k):
        for p in range(0, KC, KP):
            rows = pl.ds(k * KC + p, KP)
            yield pltpu.make_async_copy(wg_hbm.at[rows, units], wg.at[k, pl.ds(p, KP)], g_sem.at[k])
            yield pltpu.make_async_copy(wu_hbm.at[rows, units], wu.at[k, pl.ds(p, KP)], u_sem.at[k])

    def wd_copy(j):
        return pltpu.make_async_copy(wd_hbm.at[units, pl.ds(j * DB, DB)], wd.at[j], w_sem.at[j])

    def wd_pieces(j):
        for p in range(0, FH, FP):
            rows = pl.ds(pl.multiple_of(grp * FH + p, FP), FP)
            yield pltpu.make_async_copy(
                wd_hbm.at[rows, pl.ds(j * DB, DB)], wd.at[j, pl.ds(p, FP)], w_sem.at[j])

    def push(src, dst, send, recv, peer):
        return pltpu.make_async_remote_copy(src, dst, send, recv, device_id=peer, device_id_type=MESH)

    def relay_k(i, c):
        return 2 * (i // 2) + c

    def relay_cols(i, c):
        return pl.ds(pl.multiple_of(relay_k(i, c) * KC + (i % 2) * XC, XC), XC)

    def y_cols(i):
        if i < NR:
            return relay_cols(i, chip)
        return pl.ds(2 * NR * XC + (i - NR) * XC, XC)

    def y_x(i):
        c = y_cols(i)
        return push(xs.at[mine, c], xo.at[mine, c], yx_send.at[i], yx_recv.at[i], ypeer)

    def x_x(i, c):
        c = relay_cols(i, c)
        return push(xo.at[mine, c], xo.at[mine, c], xx_send.at[i], xx_recv.at[i], xpeer)

    def d_x(i):
        c = y_cols(i) if i < NR + NC else relay_cols(i - NR - NC, 1 - chip)
        return push(xo.at[mine, c], xo.at[mine, c], dx_send.at[i], dx_recv.at[i], partner)

    def on_y(i):
        y_x(i).wait_recv()
        if i < NR:
            x_x(i, chip).start()
        d_x(i).start()

    def on_x(i):
        x_x(i, 1 - chip).wait_recv()
        d_x(NR + NC + i).start()

    x_copy.start()
    def more(n):
        for _ in range(n):
            if queue:
                queue.pop(0).start()

    queue = [c for k in range(NK) for c in w_pieces(k)] + [c for j in range(ND) for c in wd_pieces(j)]
    more(8)

    barrier = pltpu.get_barrier_semaphore()
    for peer in (partner, xpeer, ypeer):
        pl.semaphore_signal(barrier, inc=1, device_id=peer, device_id_type=MESH)
    pl.semaphore_wait(barrier, 3)

    x_copy.wait()
    for i in range(NR + NC):
        y_x(i).start()
    more(8)

    def gate_up(xref, acc, k, first=False, h=None, pieces=4):
        cols = pl.ds(k * KC if isinstance(k, int) else pl.multiple_of(k * KC, KC), KC)
        for n in range(0, FH, NB):
            if (n // NB) % (8 // pieces) == 0:
                more(1)
            nn = pl.ds(n, NB)
            g = jnp.dot(xref[:, cols], wg[k, :, nn], preferred_element_type=F32)
            u = jnp.dot(xref[:, cols], wu[k, :, nn], preferred_element_type=F32)
            if not first:
                g = acc[0, :, nn] + g
                u = acc[1, :, nn] + u
            if h is None:
                acc[0, :, nn] = g
                acc[1, :, nn] = u
            else:
                h[:, nn] = (jax.nn.silu(g) * u).astype(BF16)

    def own(k):
        wait_w(k)
        gate_up(xs, acc_s, k, first=k == 0, pieces=8 if k < 4 else 4)

    def oth_y(r, first=False):
        for i in (2 * r, 2 * r + 1):
            d_x(i).wait_recv()
        gate_up(xo, acc_o, relay_k(2 * r, chip), first=first)

    def oth_x(r):
        for i in (2 * r, 2 * r + 1):
            d_x(NR + NC + i).wait_recv()
        gate_up(xo, acc_o, relay_k(2 * r, 1 - chip))

    def oth_c(r, last=False):
        for i in (2 * r, 2 * r + 1):
            d_x(NR + i).wait_recv()
        gate_up(xo, acc_o, NR + r, h=h_o if last else None)

    def wait_w(k):
        for c in w_copies(k):
            c.wait()

    own(0)
    own(1)
    on_y(0)
    own(2)
    on_y(1)
    on_y(2)
    own(3)
    on_y(3)
    oth_y(0, first=True)
    on_y(4)
    on_x(0)
    own(4)
    on_y(5)
    on_x(1)
    oth_y(1)
    on_y(6)
    on_x(2)
    own(5)
    on_y(7)
    oth_y(2)
    on_x(3)
    on_y(8)
    oth_x(0)
    on_x(4)
    on_y(9)
    on_x(5)
    wait_w(6)
    oth_c(0)
    oth_x(1)
    oth_x(2)
    wait_w(7)
    oth_c(1, last=True)

    def cols_of(j):
        return (j * DB) // FH, pl.ds((j * DB) % FH, DB)

    def term(h, acc, tb, j):
        q, cc = cols_of(j)
        acc[q, :, cc] = jnp.dot(h[...], wd[j], preferred_element_type=F32)
        tb[j] = acc[q, theirs, cc].astype(BF16)

    def core_o(j):
        return push(tb_o.at[j], rb_o.at[j], do_send.at[j], do_recv.at[j], partner)

    def core_s(j):
        return push(tb_s.at[j], rb_s.at[j], ds_send.at[j], ds_recv.at[j], partner)

    def over_y(j):
        return push(uy.at[j], yr.at[j], uy_send.at[j], uy_recv.at[j], ypeer)

    def over_x(j):
        return push(ux.at[j], xr.at[j], ux_send.at[j], ux_recv.at[j], xpeer)

    def gather(j):
        part = y_ref.at[mine, pl.ds(j * DB, DB)]
        return push(part, part, gy_send.at[j], gy_recv.at[j], partner)

    def send_y(j):
        q, cc = cols_of(j)
        core_o(j).wait_recv()
        uy[j] = (acc_o[q, mine, cc] + rb_o[j].astype(F32)).astype(BF16)
        over_y(j).start()

    def send_x(j):
        q, cc = cols_of(j)
        core_s(j).wait_recv()
        over_y(j).wait_recv()
        ux[j] = (acc_s[q, mine, cc] + rb_s[j].astype(F32) + yr[j].astype(F32)).astype(BF16)
        over_x(j).start()

    def finish(j):
        over_x(j).wait_recv()
        y_ref[mine, pl.ds(j * DB, DB)] = (ux[j].astype(F32) + xr[j].astype(F32)).astype(BF16)
        gather(j).start()

    def cross(j):
        send_x(j)
        if j >= LAG:
            finish(j - LAG)

    for j in range(ND):
        wd_copy(j).wait()
        more(4)
        term(h_o, acc_o, tb_o, j)
        core_o(j).start()
        if j >= 2:
            send_y(j - 2)
    gate_up(xs, acc_s, 6)
    send_y(ND - 2)
    send_y(ND - 1)
    gate_up(xs, acc_s, 7, h=h_s)
    for j in range(ND):
        term(h_s, acc_s, tb_s, j)
        core_s(j).start()
        if j >= LAG:
            cross(j - LAG)
    for j in range(ND - LAG, ND):
        cross(j)
    for j in range(ND - LAG, ND):
        finish(j)
    for i in range(NR + NC):
        y_x(i).wait_send()
        d_x(i).wait_send()
    for i in range(NR):
        x_x(i, chip).wait_send()
        d_x(NR + NC + i).wait_send()
    for j in range(ND):
        core_o(j).wait_send()
        core_s(j).wait_send()
        over_y(j).wait_send()
        over_x(j).wait_send()
        gather(j).wait_send()
        gather(j).wait_recv()


def mlp(x, w_gate, w_up, w_down):
    dma = pltpu.SemaphoreType.DMA
    part = pltpu.VMEM((ND, HALF, DB), BF16)
    return pl.pallas_call(
        kernel,
        name="mlp",
        out_shape=jax.ShapeDtypeStruct((ROWS, D), BF16),
        in_specs=[pl.BlockSpec(memory_space=pl.ANY)] * 4,
        out_specs=pl.BlockSpec(memory_space=pltpu.VMEM),
        scratch_shapes=[
            pltpu.VMEM((ROWS, D), BF16),
            pltpu.VMEM((ROWS, D), BF16),
            pltpu.VMEM((NK, KC, FH), BF16),
            pltpu.VMEM((NK, KC, FH), BF16),
            pltpu.VMEM((ND, FH, DB), BF16),
            pltpu.VMEM((2, ROWS, FH), F32),
            pltpu.VMEM((2, ROWS, FH), F32),
            pltpu.VMEM((ROWS, FH), BF16),
            pltpu.VMEM((ROWS, FH), BF16),
            part, part, part, part, part, part, part, part,
            dma, dma((NK,)), dma((NK,)), dma((ND,)),
            dma((NR + NC,)), dma((NR + NC,)), dma((NR,)), dma((NR,)),
            dma((2 * NR + NC,)), dma((2 * NR + NC,)),
            dma((ND,)), dma((ND,)), dma((ND,)), dma((ND,)), dma((ND,)), dma((ND,)),
            dma((ND,)), dma((ND,)), dma((ND,)), dma((ND,)),
        ],
        compiler_params=pltpu.CompilerParams(
            collective_id=0, has_side_effects=True, vmem_limit_bytes=67043328),
    )(x, w_gate, w_up, w_down)


def solution(mesh):
    return jax.shard_map(
        mlp,
        mesh=mesh,
        in_specs=(P("dp", None), P(None, "tp"), P(None, "tp"), P("tp", None)),
        out_specs=P("dp", None),
        check_vma=False,
    )
```

```python
import jax
import jax.numpy as jnp
from jax import lax
from jax.experimental import pallas as pl
from jax.experimental.pallas import tpu as pltpu
from jax.sharding import PartitionSpec as P

MESH = pl.DeviceIdType.MESH
F32 = jnp.float32
BF16 = jnp.bfloat16
ROWS = 128
HALF = ROWS // 2
D = 4096
F = 4096
FH = F // 2
KC = 512
NK = D // KC
XC = 256
NR = 6
NC = 4
NB = 256
DB = 512
ND = D // DB
KP = 128
FP = 512
XP = 16
PREFILL = 2
START = 4
WIDTHS = (256, 256, 512, 512, 512, 512, 512, 512, 256, 256)
NT = len(WIDTHS)
OFFS = tuple(sum(WIDTHS[:j]) for j in range(NT))

SCHEDULE = (
    ('i',4), ('i',1), ('i',1), ('i',1), ('i',1), ('i',1), ('i',1), ('i',1), ('i',1), ('i',1), ('i',1), ('i',1),
    ('y',0), ('i',1), ('i',1), ('s',0,0,(0,0,0,0)), ('s',0,1,(0,0,0,0)), ('y',1), ('i',4), ('i',1), ('i',1),
    ('i',1), ('y',2), ('i',1), ('s',1,0,(0,0,0,0)), ('s',1,1,(0,0,0,0)), ('y',3), ('o','y0',(0,0,1,0,1,0,0,1)),
    ('x',0), ('i',4), ('i',1), ('y',4), ('i',1), ('i',1), ('s',2,0,(0,0,0,0)), ('x',1), ('s',2,1,(0,0,0,0)),
    ('y',5), ('o','y1',(0,0,0,1,0,1,0,1)), ('y',6), ('x',2), ('s',3,0,(0,1,0,1)), ('o','x0',(0,0,1,0,1,0,1,0)),
    ('y',7), ('x',3), ('s',3,1,(1,0,1,0)), ('x',4), ('s',4,0,(1,0,0,1)), ('y',8), ('s',4,1,(0,1,0,1)),
    ('o','y2',(0,1,0,1,0,0,1,0)), ('y',9), ('x',5), ('o','x1',(1,0,1,0,1,0,1,0)), ('s',5,0,(0,1,0,1)),
    ('o','c0',(0,1,0,1,0,1,0,0)), ('o','x2',(1,0,1,0,1,0,0,1)), ('o','c1',(0,1,0,1,0,1,0,0)),
    ('s',5,1,(1,0,1,0)), ('t',0,(1,)), ('t',1,(1,)), ('t',2,(1,)), ('s',6,0,(2,0,1,0)), ('s',6,1,(1,0,1,0)),
    ('e',0), ('t',3,(0,)), ('e',1), ('s',7,0,(1,1,0,1)), ('e',2), ('s',7,1,(0,1,0,1)), ('t',4,(0,)),
    ('t',5,(1,)), ('e',3), ('S',0,(2,)), ('S',1,(2,)), ('S',2,(1,)), ('t',6,(1,)), ('e',4), ('S',3,(0,)),
    ('e',5), ('S',4,(0,)), ('c',0), ('t',7,(0,)), ('c',1), ('S',5,(0,)), ('e',6), ('t',8,(0,)), ('t',9,(0,)),
    ('S',6,(0,)), ('S',7,(0,)), ('e',7), ('c',2), ('S',8,(0,)), ('S',9,(0,)), ('e',8), ('e',9), ('f',0),
    ('c',3), ('f',1), ('c',4), ('f',2), ('c',5), ('f',3), ('c',6), ('f',4), ('c',7), ('f',5), ('c',8), ('c',9),
    ('f',6), ('f',7), ('f',8), ('f',9),
)


def kernel(x_hbm, wg_hbm, wu_hbm, wd_hbm, y_ref,
           xs, xo, wg, wu, wd, acc_s, acc_o, h_s, h_o,
           tb_o, rb_o, uy, yr, tb_s, rb_s, ux, xr,
           x_sem, g_sem, u_sem, w_sem,
           yx_send, yx_recv, xx_send, xx_recv, dx_send, dx_recv,
           do_send, do_recv, uy_send, uy_recv, ds_send, ds_recv,
           ux_send, ux_recv, gy_send, gy_recv):
    grp = lax.axis_index("dp")
    tp = lax.axis_index("tp")
    core = lax.rem(tp, 2)
    chip = tp // 2
    partner = {"tp": 2 * chip + (1 - core)}
    xpeer = {"tp": 2 * (1 - chip) + core}
    ypeer = {"dp": 1 - grp}
    mine = pl.ds(pl.multiple_of(core * HALF, HALF), HALF)
    theirs = pl.ds(pl.multiple_of((1 - core) * HALF, HALF), HALF)
    units = pl.ds(pl.multiple_of(grp * FH, FH), FH)

    barrier = pltpu.get_barrier_semaphore()
    for peer in (partner, xpeer, ypeer):
        pl.semaphore_signal(barrier, inc=1, device_id=peer, device_id_type=MESH)

    for p in range(0, HALF, XP):
        rows = pl.ds(pl.multiple_of(core * HALF + p, XP), XP)
        pltpu.make_async_copy(x_hbm.at[rows], xs.at[rows], x_sem.at[0]).start()
    x_mine = pltpu.make_async_copy(x_hbm.at[mine], xs.at[mine], x_sem.at[0])
    x_theirs = pltpu.make_async_copy(x_hbm.at[theirs], xs.at[theirs], x_sem.at[1])

    def w_copies(k):
        rows = pl.ds(k * KC, KC)
        return (pltpu.make_async_copy(wg_hbm.at[rows, units], wg.at[k], g_sem.at[k]),
                pltpu.make_async_copy(wu_hbm.at[rows, units], wu.at[k], u_sem.at[k]))

    def w_pieces(k):
        for p in range(0, KC, KP):
            rows = pl.ds(k * KC + p, KP)
            yield pltpu.make_async_copy(wg_hbm.at[rows, units], wg.at[k, pl.ds(p, KP)], g_sem.at[k])
            yield pltpu.make_async_copy(wu_hbm.at[rows, units], wu.at[k, pl.ds(p, KP)], u_sem.at[k])

    def wd_copy(j):
        return pltpu.make_async_copy(wd_hbm.at[units, pl.ds(j * DB, DB)], wd.at[j], w_sem.at[j])

    def wd_pieces(j):
        for p in range(0, FH, FP):
            rows = pl.ds(pl.multiple_of(grp * FH + p, FP), FP)
            yield pltpu.make_async_copy(
                wd_hbm.at[rows, pl.ds(j * DB, DB)], wd.at[j, pl.ds(p, FP)], w_sem.at[j])

    queue = [c for k in range(NK) for c in w_pieces(k)] + [c for j in range(ND) for c in wd_pieces(j)]

    def more(n):
        for _ in range(n):
            if queue:
                queue.pop(0).start()

    def push(src, dst, send, recv, peer):
        return pltpu.make_async_remote_copy(src, dst, send, recv, device_id=peer, device_id_type=MESH)

    def relay_k(i, c):
        return 2 * (i // 2) + c

    def relay_cols(i, c):
        return pl.ds(pl.multiple_of(relay_k(i, c) * KC + (i % 2) * XC, XC), XC)

    def y_cols(i):
        if i < NR:
            return relay_cols(i, chip)
        return pl.ds(2 * NR * XC + (i - NR) * XC, XC)

    def y_x(i):
        c = y_cols(i)
        return push(xs.at[mine, c], xo.at[mine, c], yx_send.at[i], yx_recv.at[i], ypeer)

    def x_x(i, c):
        c = relay_cols(i, c)
        return push(xo.at[mine, c], xo.at[mine, c], xx_send.at[i], xx_recv.at[i], xpeer)

    def d_x(i):
        c = y_cols(i) if i < NR + NC else relay_cols(i - NR - NC, 1 - chip)
        return push(xo.at[mine, c], xo.at[mine, c], dx_send.at[i], dx_recv.at[i], partner)

    def on_y(i):
        y_x(i).wait_recv()
        if i < NR:
            x_x(i, chip).start()
        d_x(i).start()

    def on_x(i):
        x_x(i, 1 - chip).wait_recv()
        d_x(NR + NC + i).start()

    waited = set()

    def wait_w(*ks):
        for k in ks:
            if k not in waited:
                waited.add(k)
                for c in w_copies(k):
                    c.wait()

    def wait_wd(j):
        if ("d", j) not in waited:
            waited.add(("d", j))
            wd_copy(j).wait()

    def gate_up(xref, acc, k, lo, hi, counts, first, h):
        cols = pl.ds(k * KC if isinstance(k, int) else pl.multiple_of(k * KC, KC), KC)
        for n in range(lo, hi, NB):
            more(counts[(n - lo) // NB])
            nn = pl.ds(n, NB)
            g = jnp.dot(xref[:, cols], wg[k, :, nn], preferred_element_type=F32)
            u = jnp.dot(xref[:, cols], wu[k, :, nn], preferred_element_type=F32)
            if not first:
                g = acc[0, :, nn] + g
                u = acc[1, :, nn] + u
            if h is None:
                acc[0, :, nn] = g
                acc[1, :, nn] = u
            else:
                h[:, nn] = (jax.nn.silu(g) * u).astype(BF16)

    def own(k, half, counts):
        wait_w(k)
        if "x" not in waited:
            waited.add("x")
            x_theirs.wait()
        lo = half * (FH // 2)
        gate_up(xs, acc_s, k, lo, lo + FH // 2, counts, k == 0, h_s if k == NK - 1 else None)

    slots = [t[1] for t in SCHEDULE if t[0] == "o"]

    def other(slot, counts):
        kind, r = slot[0], int(slot[1])
        if kind == "c":
            wait_w(NR + r)
            k = NR + r
            ready = (NR + 2 * r, NR + 2 * r + 1)
        else:
            wait_w(2 * r, 2 * r + 1)
            k = relay_k(2 * r, chip if kind == "y" else 1 - chip)
            base = 0 if kind == "y" else NR + NC
            ready = (base + 2 * r, base + 2 * r + 1)
        for i in ready:
            d_x(i).wait_recv()
        gate_up(xo, acc_o, k, 0, FH, counts, slot == slots[0], h_o if slot == slots[-1] else None)

    def block(j):
        return pl.ds(OFFS[j], WIDTHS[j])

    def term(h, acc, tb, j, counts):
        o, w = OFFS[j], WIDTHS[j]
        wait_wd(o // DB)
        more(counts[0])
        acc[o // FH, :, pl.ds(o % FH, w)] = jnp.dot(
            h[...], wd[o // DB, :, pl.ds(o % DB, w)], preferred_element_type=F32)
        tb[:, block(j)] = acc[o // FH, theirs, pl.ds(o % FH, w)].astype(BF16)

    def part(acc, j):
        o, w = OFFS[j], WIDTHS[j]
        return acc[o // FH, mine, pl.ds(o % FH, w)]

    def core_o(j):
        return push(tb_o.at[:, block(j)], rb_o.at[:, block(j)], do_send.at[j], do_recv.at[j], partner)

    def core_s(j):
        return push(tb_s.at[:, block(j)], rb_s.at[:, block(j)], ds_send.at[j], ds_recv.at[j], partner)

    def over_y(j):
        return push(uy.at[:, block(j)], yr.at[:, block(j)], uy_send.at[j], uy_recv.at[j], ypeer)

    def over_x(j):
        return push(ux.at[:, block(j)], xr.at[:, block(j)], ux_send.at[j], ux_recv.at[j], xpeer)

    def gather(j):
        rows = y_ref.at[mine, block(j)]
        return push(rows, rows, gy_send.at[j], gy_recv.at[j], partner)

    def send_y(j):
        core_o(j).wait_recv()
        uy[:, block(j)] = (part(acc_o, j) + rb_o[:, block(j)].astype(F32)).astype(BF16)
        over_y(j).start()

    def send_x(j):
        core_s(j).wait_recv()
        over_y(j).wait_recv()
        ux[:, block(j)] = (part(acc_s, j) + rb_s[:, block(j)].astype(F32)
                           + yr[:, block(j)].astype(F32)).astype(BF16)
        over_x(j).start()

    def finish(j):
        over_x(j).wait_recv()
        y_ref[mine, block(j)] = (ux[:, block(j)].astype(F32) + xr[:, block(j)].astype(F32)).astype(BF16)
        gather(j).start()

    more(PREFILL)
    pl.semaphore_wait(barrier, 3)
    x_mine.wait()
    for i in range(NR + NC):
        y_x(i).start()
    x_theirs.start()
    more(START)

    for kind, i, *rest in SCHEDULE:
        if kind == "y":
            on_y(i)
        elif kind == "x":
            on_x(i)
        elif kind == "s":
            own(i, *rest)
        elif kind == "o":
            other(i, *rest)
        elif kind == "t":
            term(h_o, acc_o, tb_o, i, *rest)
            core_o(i).start()
        elif kind == "S":
            term(h_s, acc_s, tb_s, i, *rest)
            core_s(i).start()
        elif kind == "e":
            send_y(i)
        elif kind == "c":
            send_x(i)
        elif kind == "f":
            finish(i)
        else:
            more(i)

    for j in range(NT):
        gather(j).wait_recv()
    for i in range(NR + NC):
        y_x(i).wait_send()
        d_x(i).wait_send()
    for i in range(NR):
        x_x(i, chip).wait_send()
        d_x(NR + NC + i).wait_send()
    for j in range(NT):
        core_o(j).wait_send()
        core_s(j).wait_send()
        over_y(j).wait_send()
        over_x(j).wait_send()
        gather(j).wait_send()


def mlp(x, w_gate, w_up, w_down):
    dma = pltpu.SemaphoreType.DMA
    half = pltpu.VMEM((HALF, D), BF16)
    return pl.pallas_call(
        kernel,
        name="mlp",
        out_shape=jax.ShapeDtypeStruct((ROWS, D), BF16),
        in_specs=[pl.BlockSpec(memory_space=pl.ANY)] * 4,
        out_specs=pl.BlockSpec(memory_space=pltpu.VMEM),
        scratch_shapes=[
            pltpu.VMEM((ROWS, D), BF16),
            pltpu.VMEM((ROWS, D), BF16),
            pltpu.VMEM((NK, KC, FH), BF16),
            pltpu.VMEM((NK, KC, FH), BF16),
            pltpu.VMEM((ND, FH, DB), BF16),
            pltpu.VMEM((2, ROWS, FH), F32),
            pltpu.VMEM((2, ROWS, FH), F32),
            pltpu.VMEM((ROWS, FH), BF16),
            pltpu.VMEM((ROWS, FH), BF16),
            half, half, half, half, half, half, half, half,
            dma((2,)), dma((NK,)), dma((NK,)), dma((ND,)),
            dma((NR + NC,)), dma((NR + NC,)), dma((NR,)), dma((NR,)),
            dma((2 * NR + NC,)), dma((2 * NR + NC,)),
            dma((NT,)), dma((NT,)), dma((NT,)), dma((NT,)), dma((NT,)), dma((NT,)),
            dma((NT,)), dma((NT,)), dma((NT,)), dma((NT,)),
        ],
        compiler_params=pltpu.CompilerParams(
            collective_id=0, has_side_effects=True, vmem_limit_bytes=67043328),
    )(x, w_gate, w_up, w_down)


def solution(mesh):
    return jax.shard_map(
        mlp,
        mesh=mesh,
        in_specs=(P("dp", None), P(None, "tp"), P(None, "tp"), P("tp", None)),
        out_specs=P("dp", None),
        check_vma=False,
    )
```

```python
import jax
import jax.numpy as jnp
from jax import lax
from jax.experimental import pallas as pl
from jax.experimental.pallas import tpu as pltpu
from jax.sharding import PartitionSpec as P

MESH = pl.DeviceIdType.MESH
F32 = jnp.float32
BF16 = jnp.bfloat16
ROWS = 128
HALF = ROWS // 2
D = 4096
F = 4096
FH = F // 2
KC = 512
NK = D // KC
XC = 256
NR = 6
NC = 4
NB = 256
DB = 512
ND = D // DB
XP = 16
WIDTHS = (256, 256, 512, 512, 512, 512, 512, 512, 256, 256)
NT = len(WIDTHS)
OFFS = tuple(sum(WIDTHS[:j]) for j in range(NT))

SCHEDULE = (
    ('s',0,0), ('s',0,1), ('y',0), ('s',1,0), ('s',1,1), ('y',1), ('y',2), ('s',2,0), ('s',2,1), ('y',3),
    ('o','y0'), ('y',4), ('x',0), ('s',3,0), ('o','y1'), ('y',5), ('x',1), ('s',3,1), ('y',6), ('x',2),
    ('s',4,0), ('s',4,1), ('y',7), ('x',3), ('o','x0'), ('y',8), ('x',4), ('o','y2'), ('y',9), ('x',5),
    ('o','x1'), ('o','c0'), ('o','x2'), ('o','c1'), ('t',0), ('t',1), ('t',2), ('s',5,0), ('s',5,1), ('e',0),
    ('e',1), ('s',6,0), ('t',3), ('e',2), ('s',6,1), ('s',7,0), ('s',7,1), ('t',4), ('e',3), ('S',0), ('S',1),
    ('S',2), ('t',5), ('e',4), ('S',3), ('c',0), ('c',1), ('S',4), ('S',5), ('c',2), ('t',6), ('e',5), ('S',6),
    ('t',7), ('S',7), ('c',3), ('t',8), ('e',6), ('f',0), ('S',8), ('t',9), ('e',7), ('S',9), ('f',1), ('c',4),
    ('e',8), ('e',9), ('f',2), ('c',5), ('f',3), ('c',6), ('f',4), ('c',7), ('c',8), ('f',5), ('c',9), ('f',6),
    ('f',7), ('f',8), ('f',9),
)


def kernel(x_hbm, wg_hbm, wu_hbm, wd_hbm, y_ref,
           xs, xo, wg, wu, wd, acc_s, acc_o, h_s, h_o,
           tb_o, rb_o, uy, yr, tb_s, rb_s, ux, xr,
           f_sem, x_sem, g_sem, u_sem, w_sem,
           yx_send, yx_recv, xx_send, xx_recv, dx_send, dx_recv,
           do_send, do_recv, uy_send, uy_recv, ds_send, ds_recv,
           ux_send, ux_recv, gy_send, gy_recv):
    grp = lax.axis_index("dp")
    tp = lax.axis_index("tp")
    core = lax.rem(tp, 2)
    chip = tp // 2
    partner = {"tp": 2 * chip + (1 - core)}
    xpeer = {"tp": 2 * (1 - chip) + core}
    ypeer = {"dp": 1 - grp}
    mine = pl.ds(pl.multiple_of(core * HALF, HALF), HALF)
    theirs = pl.ds(pl.multiple_of((1 - core) * HALF, HALF), HALF)
    units = pl.ds(pl.multiple_of(grp * FH, FH), FH)

    def fence():
        pl.semaphore_signal(f_sem, 1)
        pl.semaphore_wait(f_sem, 1)

    barrier = pltpu.get_barrier_semaphore()
    for peer in (partner, xpeer, ypeer):
        pl.semaphore_signal(barrier, inc=1, device_id=peer, device_id_type=MESH)

    for p in range(0, HALF, XP):
        rows = pl.ds(pl.multiple_of(core * HALF + p, XP), XP)
        pltpu.make_async_copy(x_hbm.at[rows], xs.at[rows], x_sem.at[0]).start()
    x_mine = pltpu.make_async_copy(x_hbm.at[mine], xs.at[mine], x_sem.at[0])
    x_theirs = pltpu.make_async_copy(x_hbm.at[theirs], xs.at[theirs], x_sem.at[1])

    def w_copies(k):
        rows = pl.ds(k * KC, KC)
        return (pltpu.make_async_copy(wg_hbm.at[rows, units], wg.at[k], g_sem.at[k]),
                pltpu.make_async_copy(wu_hbm.at[rows, units], wu.at[k], u_sem.at[k]))

    def wd_copy(j):
        return pltpu.make_async_copy(wd_hbm.at[units, pl.ds(j * DB, DB)], wd.at[j], w_sem.at[j])

    def push(src, dst, send, recv, peer):
        return pltpu.make_async_remote_copy(src, dst, send, recv, device_id=peer, device_id_type=MESH)

    def relay_k(i, c):
        return 2 * (i // 2) + c

    def relay_cols(i, c):
        return pl.ds(pl.multiple_of(relay_k(i, c) * KC + (i % 2) * XC, XC), XC)

    def y_cols(i):
        if i < NR:
            return relay_cols(i, chip)
        return pl.ds(2 * NR * XC + (i - NR) * XC, XC)

    def y_x(i):
        c = y_cols(i)
        return push(xs.at[mine, c], xo.at[mine, c], yx_send.at[i], yx_recv.at[i], ypeer)

    def x_x(i, c):
        c = relay_cols(i, c)
        return push(xo.at[mine, c], xo.at[mine, c], xx_send.at[i], xx_recv.at[i], xpeer)

    def d_x(i):
        c = y_cols(i) if i < NR + NC else relay_cols(i - NR - NC, 1 - chip)
        return push(xo.at[mine, c], xo.at[mine, c], dx_send.at[i], dx_recv.at[i], partner)

    def on_y(i):
        y_x(i).wait_recv()
        if i < NR:
            x_x(i, chip).start()
        d_x(i).start()

    def on_x(i):
        x_x(i, 1 - chip).wait_recv()
        d_x(NR + NC + i).start()

    waited = set()

    def wait_w(*ks):
        for k in ks:
            if k not in waited:
                waited.add(k)
                for c in w_copies(k):
                    c.wait()

    def wait_wd(j):
        if ("d", j) not in waited:
            waited.add(("d", j))
            wd_copy(j).wait()

    def gate_up(xref, acc, k, lo, hi, first, h):
        cols = pl.ds(k * KC if isinstance(k, int) else pl.multiple_of(k * KC, KC), KC)
        for n in range(lo, hi, NB):
            nn = pl.ds(n, NB)
            g = jnp.dot(xref[:, cols], wg[k, :, nn], preferred_element_type=F32)
            u = jnp.dot(xref[:, cols], wu[k, :, nn], preferred_element_type=F32)
            if not first:
                g = acc[0, :, nn] + g
                u = acc[1, :, nn] + u
            if h is None:
                acc[0, :, nn] = g
                acc[1, :, nn] = u
            else:
                h[:, nn] = (jax.nn.silu(g) * u).astype(BF16)

    def own(k, half):
        wait_w(k)
        if "x" not in waited:
            waited.add("x")
            x_theirs.wait()
        lo = half * (FH // 2)
        gate_up(xs, acc_s, k, lo, lo + FH // 2, k == 0, h_s if k == NK - 1 else None)

    slots = [t[1] for t in SCHEDULE if t[0] == "o"]

    def other(slot):
        kind, r = slot[0], int(slot[1])
        if kind == "c":
            wait_w(NR + r)
            k = NR + r
            ready = (NR + 2 * r, NR + 2 * r + 1)
        else:
            wait_w(2 * r, 2 * r + 1)
            k = relay_k(2 * r, chip if kind == "y" else 1 - chip)
            base = 0 if kind == "y" else NR + NC
            ready = (base + 2 * r, base + 2 * r + 1)
        for i in ready:
            d_x(i).wait_recv()
        gate_up(xo, acc_o, k, 0, FH, slot == slots[0], h_o if slot == slots[-1] else None)

    def block(j):
        return pl.ds(OFFS[j], WIDTHS[j])

    def term(h, acc, tb, j):
        o, w = OFFS[j], WIDTHS[j]
        wait_wd(o // DB)
        acc[o // FH, :, pl.ds(o % FH, w)] = jnp.dot(
            h[...], wd[o // DB, :, pl.ds(o % DB, w)], preferred_element_type=F32)
        tb[:, block(j)] = acc[o // FH, theirs, pl.ds(o % FH, w)].astype(BF16)

    def part(acc, j):
        o, w = OFFS[j], WIDTHS[j]
        return acc[o // FH, mine, pl.ds(o % FH, w)]

    def core_o(j):
        return push(tb_o.at[:, block(j)], rb_o.at[:, block(j)], do_send.at[j], do_recv.at[j], partner)

    def core_s(j):
        return push(tb_s.at[:, block(j)], rb_s.at[:, block(j)], ds_send.at[j], ds_recv.at[j], partner)

    def over_y(j):
        return push(uy.at[:, block(j)], yr.at[:, block(j)], uy_send.at[j], uy_recv.at[j], ypeer)

    def over_x(j):
        return push(ux.at[:, block(j)], xr.at[:, block(j)], ux_send.at[j], ux_recv.at[j], xpeer)

    def gather(j):
        rows = y_ref.at[mine, block(j)]
        return push(rows, rows, gy_send.at[j], gy_recv.at[j], partner)

    def send_y(j):
        core_o(j).wait_recv()
        uy[:, block(j)] = (part(acc_o, j) + rb_o[:, block(j)].astype(F32)).astype(BF16)
        over_y(j).start()

    def send_x(j):
        core_s(j).wait_recv()
        over_y(j).wait_recv()
        ux[:, block(j)] = (part(acc_s, j) + rb_s[:, block(j)].astype(F32)
                           + yr[:, block(j)].astype(F32)).astype(BF16)
        over_x(j).start()

    def finish(j):
        over_x(j).wait_recv()
        y_ref[mine, block(j)] = (ux[:, block(j)].astype(F32) + xr[:, block(j)].astype(F32)).astype(BF16)
        gather(j).start()

    fence()
    for k in range(NK):
        for c in w_copies(k):
            c.start()
        if k == 0:
            fence()
            x_theirs.start()
        fence()
    for j in range(ND):
        wd_copy(j).start()
    pl.semaphore_wait(barrier, 3)
    x_mine.wait()
    for i in range(NR + NC):
        y_x(i).start()

    for kind, i, *rest in SCHEDULE:
        if kind == "y":
            on_y(i)
        elif kind == "x":
            on_x(i)
        elif kind == "s":
            own(i, *rest)
        elif kind == "o":
            other(i, *rest)
        elif kind == "t":
            term(h_o, acc_o, tb_o, i, *rest)
            core_o(i).start()
        elif kind == "S":
            term(h_s, acc_s, tb_s, i, *rest)
            core_s(i).start()
        elif kind == "e":
            send_y(i)
        elif kind == "c":
            send_x(i)
        else:
            finish(i)

    for j in range(NT):
        gather(j).wait_recv()
    for i in range(NR + NC):
        y_x(i).wait_send()
        d_x(i).wait_send()
    for i in range(NR):
        x_x(i, chip).wait_send()
        d_x(NR + NC + i).wait_send()
    for j in range(NT):
        core_o(j).wait_send()
        core_s(j).wait_send()
        over_y(j).wait_send()
        over_x(j).wait_send()
        gather(j).wait_send()


def mlp(x, w_gate, w_up, w_down):
    dma = pltpu.SemaphoreType.DMA
    half = pltpu.VMEM((HALF, D), BF16)
    return pl.pallas_call(
        kernel,
        name="mlp",
        out_shape=jax.ShapeDtypeStruct((ROWS, D), BF16),
        in_specs=[pl.BlockSpec(memory_space=pl.ANY)] * 4,
        out_specs=pl.BlockSpec(memory_space=pltpu.VMEM),
        scratch_shapes=[
            pltpu.VMEM((ROWS, D), BF16),
            pltpu.VMEM((ROWS, D), BF16),
            pltpu.VMEM((NK, KC, FH), BF16),
            pltpu.VMEM((NK, KC, FH), BF16),
            pltpu.VMEM((ND, FH, DB), BF16),
            pltpu.VMEM((2, ROWS, FH), F32),
            pltpu.VMEM((2, ROWS, FH), F32),
            pltpu.VMEM((ROWS, FH), BF16),
            pltpu.VMEM((ROWS, FH), BF16),
            half, half, half, half, half, half, half, half,
            pltpu.SemaphoreType.REGULAR,
            dma((2,)), dma((NK,)), dma((NK,)), dma((ND,)),
            dma((NR + NC,)), dma((NR + NC,)), dma((NR,)), dma((NR,)),
            dma((2 * NR + NC,)), dma((2 * NR + NC,)),
            dma((NT,)), dma((NT,)), dma((NT,)), dma((NT,)), dma((NT,)), dma((NT,)),
            dma((NT,)), dma((NT,)), dma((NT,)), dma((NT,)),
        ],
        compiler_params=pltpu.CompilerParams(
            collective_id=0, has_side_effects=True, vmem_limit_bytes=67043328),
    )(x, w_gate, w_up, w_down)


def solution(mesh):
    return jax.shard_map(
        mlp,
        mesh=mesh,
        in_specs=(P("dp", None), P(None, "tp"), P(None, "tp"), P("tp", None)),
        out_specs=P("dp", None),
        check_vma=False,
    )
```

```python
import jax
import jax.numpy as jnp
from jax import lax
from jax.experimental import pallas as pl
from jax.experimental.pallas import tpu as pltpu
from jax.sharding import PartitionSpec as P

MESH = pl.DeviceIdType.MESH
F32 = jnp.float32
BF16 = jnp.bfloat16
ROWS = 128
HALF = ROWS // 2
D = 4096
F = 4096
FH = F // 2
KC = 512
NK = D // KC
XC = 256
NR = 6
NC = 4
NB = 256
DB = 512
ND = D // DB
XP = 16
WIDTHS = (256, 256, 512, 512, 512, 512, 512, 512, 256, 256)
NT = len(WIDTHS)
OFFS = tuple(sum(WIDTHS[:j]) for j in range(NT))

SCHEDULE = (
    ('s',0,0), ('s',0,1), ('s',1,0), ('y',0), ('s',1,1), ('y',1), ('s',2,0), ('y',2), ('s',2,1), ('y',3),
    ('s',3,0), ('o','y0'), ('y',4), ('x',0), ('s',3,1), ('y',5), ('x',1), ('o','y1'), ('y',6), ('x',2),
    ('s',4,0), ('y',7), ('s',4,1), ('x',3), ('s',5,0), ('y',8), ('o','y2'), ('y',9), ('x',4), ('o','x0'),
    ('x',5), ('o','x1'), ('o','c0'), ('o','c1'), ('o','x2'), ('t',0), ('t',1), ('t',2), ('s',5,1), ('s',6,0),
    ('s',6,1), ('e',0), ('e',1), ('s',7,0), ('t',3), ('e',2), ('s',7,1), ('S',0), ('S',1), ('t',4), ('S',2),
    ('e',3), ('S',3), ('t',5), ('c',0), ('S',4), ('c',1), ('S',5), ('e',4), ('t',6), ('S',6), ('c',2), ('t',7),
    ('e',5), ('S',7), ('t',8), ('S',8), ('e',6), ('c',3), ('f',0), ('t',9), ('S',9), ('f',1), ('e',7), ('e',8),
    ('c',4), ('e',9), ('c',5), ('f',2), ('c',6), ('f',3), ('c',7), ('f',4), ('c',8), ('f',5), ('c',9), ('f',6),
    ('f',7), ('f',8), ('f',9),
)


def kernel(x_hbm, wg_hbm, wu_hbm, wd_hbm, y_ref,
           xs, xo, wg, wu, wd, acc_s, acc_o, h_s, h_o,
           tb_o, rb_o, uy, yr, tb_s, rb_s, ux, xr,
           f_sem, x_sem, g_sem, u_sem, w_sem,
           yx_send, yx_recv, xx_send, xx_recv, dx_send, dx_recv,
           do_send, do_recv, uy_send, uy_recv, ds_send, ds_recv,
           ux_send, ux_recv, gy_send, gy_recv):
    grp = lax.axis_index("dp")
    tp = lax.axis_index("tp")
    core = lax.rem(tp, 2)
    chip = tp // 2
    partner = {"tp": 2 * chip + (1 - core)}
    xpeer = {"tp": 2 * (1 - chip) + core}
    ypeer = {"dp": 1 - grp}
    mine = pl.ds(pl.multiple_of(core * HALF, HALF), HALF)
    theirs = pl.ds(pl.multiple_of((1 - core) * HALF, HALF), HALF)
    units = pl.ds(pl.multiple_of(grp * FH, FH), FH)

    def fence():
        pl.semaphore_signal(f_sem, 1)
        pl.semaphore_wait(f_sem, 1)

    barrier = pltpu.get_barrier_semaphore()
    for peer in (partner, xpeer, ypeer):
        pl.semaphore_signal(barrier, inc=1, device_id=peer, device_id_type=MESH)

    for p in range(0, HALF, XP):
        rows = pl.ds(pl.multiple_of(core * HALF + p, XP), XP)
        pltpu.make_async_copy(x_hbm.at[rows], xs.at[rows], x_sem.at[0]).start()
    x_mine = pltpu.make_async_copy(x_hbm.at[mine], xs.at[mine], x_sem.at[0])
    x_theirs = pltpu.make_async_copy(x_hbm.at[theirs], xs.at[theirs], x_sem.at[1])

    def w_copies(k):
        rows = pl.ds(k * KC, KC)
        return (pltpu.make_async_copy(wg_hbm.at[rows, units], wg.at[k], g_sem.at[k]),
                pltpu.make_async_copy(wu_hbm.at[rows, units], wu.at[k], u_sem.at[k]))

    def wd_copy(j):
        return pltpu.make_async_copy(wd_hbm.at[units, pl.ds(j * DB, DB)], wd.at[j], w_sem.at[j])

    def push(src, dst, send, recv, peer):
        return pltpu.make_async_remote_copy(src, dst, send, recv, device_id=peer, device_id_type=MESH)

    def relay_k(i, c):
        return 2 * (i // 2) + c

    def relay_cols(i, c):
        return pl.ds(pl.multiple_of(relay_k(i, c) * KC + (i % 2) * XC, XC), XC)

    def y_cols(i):
        if i < NR:
            return relay_cols(i, chip)
        return pl.ds(2 * NR * XC + (i - NR) * XC, XC)

    def y_x(i):
        c = y_cols(i)
        return push(xs.at[mine, c], xo.at[mine, c], yx_send.at[i], yx_recv.at[i], ypeer)

    def x_x(i, c):
        c = relay_cols(i, c)
        return push(xo.at[mine, c], xo.at[mine, c], xx_send.at[i], xx_recv.at[i], xpeer)

    def d_x(i):
        c = y_cols(i) if i < NR + NC else relay_cols(i - NR - NC, 1 - chip)
        return push(xo.at[mine, c], xo.at[mine, c], dx_send.at[i], dx_recv.at[i], partner)

    def on_y(i):
        y_x(i).wait_recv()
        if i < NR:
            x_x(i, chip).start()
        d_x(i).start()

    def on_x(i):
        x_x(i, 1 - chip).wait_recv()
        d_x(NR + NC + i).start()

    waited = set()

    def wait_w(*ks):
        for k in ks:
            if k not in waited:
                waited.add(k)
                for c in w_copies(k):
                    c.wait()

    def wait_wd(j):
        if ("d", j) not in waited:
            waited.add(("d", j))
            wd_copy(j).wait()

    def gate_up(xref, acc, k, lo, hi, first, h):
        cols = pl.ds(k * KC if isinstance(k, int) else pl.multiple_of(k * KC, KC), KC)
        for n in range(lo, hi, NB):
            nn = pl.ds(n, NB)
            g = jnp.dot(xref[:, cols], wg[k, :, nn], preferred_element_type=F32)
            u = jnp.dot(xref[:, cols], wu[k, :, nn], preferred_element_type=F32)
            if not first:
                g = acc[0, :, nn] + g
                u = acc[1, :, nn] + u
            if h is None:
                acc[0, :, nn] = g
                acc[1, :, nn] = u
            else:
                h[:, nn] = (jax.nn.silu(g) * u).astype(BF16)

    def own(k, half):
        wait_w(k)
        if "x" not in waited:
            waited.add("x")
            x_theirs.wait()
        lo = half * (FH // 2)
        gate_up(xs, acc_s, k, lo, lo + FH // 2, k == 0, h_s if k == NK - 1 else None)

    slots = [t[1] for t in SCHEDULE if t[0] == "o"]

    def other(slot):
        kind, r = slot[0], int(slot[1])
        if kind == "c":
            wait_w(NR + r)
            k = NR + r
            ready = (NR + 2 * r, NR + 2 * r + 1)
        else:
            wait_w(2 * r, 2 * r + 1)
            k = relay_k(2 * r, chip if kind == "y" else 1 - chip)
            base = 0 if kind == "y" else NR + NC
            ready = (base + 2 * r, base + 2 * r + 1)
        for i in ready:
            d_x(i).wait_recv()
        gate_up(xo, acc_o, k, 0, FH, slot == slots[0], h_o if slot == slots[-1] else None)

    def block(j):
        return pl.ds(OFFS[j], WIDTHS[j])

    def term(h, acc, tb, j):
        o, w = OFFS[j], WIDTHS[j]
        wait_wd(o // DB)
        acc[o // FH, :, pl.ds(o % FH, w)] = jnp.dot(
            h[...], wd[o // DB, :, pl.ds(o % DB, w)], preferred_element_type=F32)
        tb[:, block(j)] = acc[o // FH, theirs, pl.ds(o % FH, w)].astype(BF16)

    def part(acc, j):
        o, w = OFFS[j], WIDTHS[j]
        return acc[o // FH, mine, pl.ds(o % FH, w)]

    def core_o(j):
        return push(tb_o.at[:, block(j)], rb_o.at[:, block(j)], do_send.at[j], do_recv.at[j], partner)

    def core_s(j):
        return push(tb_s.at[:, block(j)], rb_s.at[:, block(j)], ds_send.at[j], ds_recv.at[j], partner)

    def over_y(j):
        return push(uy.at[:, block(j)], yr.at[:, block(j)], uy_send.at[j], uy_recv.at[j], ypeer)

    def over_x(j):
        return push(ux.at[:, block(j)], xr.at[:, block(j)], ux_send.at[j], ux_recv.at[j], xpeer)

    def gather(j):
        rows = y_ref.at[mine, block(j)]
        return push(rows, rows, gy_send.at[j], gy_recv.at[j], partner)

    def send_y(j):
        core_o(j).wait_recv()
        uy[:, block(j)] = (part(acc_o, j) + rb_o[:, block(j)].astype(F32)).astype(BF16)
        over_y(j).start()

    def send_x(j):
        core_s(j).wait_recv()
        over_y(j).wait_recv()
        ux[:, block(j)] = (part(acc_s, j) + rb_s[:, block(j)].astype(F32)
                           + yr[:, block(j)].astype(F32)).astype(BF16)
        over_x(j).start()

    def finish(j):
        over_x(j).wait_recv()
        y_ref[mine, block(j)] = (ux[:, block(j)].astype(F32) + xr[:, block(j)].astype(F32)).astype(BF16)
        gather(j).start()

    fence()
    for k in range(NK):
        for c in w_copies(k):
            c.start()
        if k == 0:
            fence()
            x_theirs.start()
        fence()
    for j in range(ND):
        wd_copy(j).start()
    pl.semaphore_wait(barrier, 3)
    x_mine.wait()
    for i in range(NR + NC):
        y_x(i).start()

    for kind, i, *rest in SCHEDULE:
        if kind == "y":
            on_y(i)
        elif kind == "x":
            on_x(i)
        elif kind == "s":
            own(i, *rest)
        elif kind == "o":
            other(i, *rest)
        elif kind == "t":
            term(h_o, acc_o, tb_o, i, *rest)
            core_o(i).start()
        elif kind == "S":
            term(h_s, acc_s, tb_s, i, *rest)
            core_s(i).start()
        elif kind == "e":
            send_y(i)
        elif kind == "c":
            send_x(i)
        else:
            finish(i)

    for j in range(NT):
        gather(j).wait_recv()
    for i in range(NR + NC):
        y_x(i).wait_send()
        d_x(i).wait_send()
    for i in range(NR):
        x_x(i, chip).wait_send()
        d_x(NR + NC + i).wait_send()
    for j in range(NT):
        core_o(j).wait_send()
        core_s(j).wait_send()
        over_y(j).wait_send()
        over_x(j).wait_send()
        gather(j).wait_send()


def mlp(x, w_gate, w_up, w_down):
    dma = pltpu.SemaphoreType.DMA
    half = pltpu.VMEM((HALF, D), BF16)
    return pl.pallas_call(
        kernel,
        name="mlp",
        out_shape=pltpu.VMEM((ROWS, D), BF16),
        in_specs=[pl.BlockSpec(memory_space=pl.ANY)] * 4,
        out_specs=pl.BlockSpec(memory_space=pltpu.VMEM),
        scratch_shapes=[
            pltpu.VMEM((ROWS, D), BF16),
            pltpu.VMEM((ROWS, D), BF16),
            pltpu.VMEM((NK, KC, FH), BF16),
            pltpu.VMEM((NK, KC, FH), BF16),
            pltpu.VMEM((ND, FH, DB), BF16),
            pltpu.VMEM((2, ROWS, FH), F32),
            pltpu.VMEM((2, ROWS, FH), F32),
            pltpu.VMEM((ROWS, FH), BF16),
            pltpu.VMEM((ROWS, FH), BF16),
            half, half, half, half, half, half, half, half,
            pltpu.SemaphoreType.REGULAR,
            dma((2,)), dma((NK,)), dma((NK,)), dma((ND,)),
            dma((NR + NC,)), dma((NR + NC,)), dma((NR,)), dma((NR,)),
            dma((2 * NR + NC,)), dma((2 * NR + NC,)),
            dma((NT,)), dma((NT,)), dma((NT,)), dma((NT,)), dma((NT,)), dma((NT,)),
            dma((NT,)), dma((NT,)), dma((NT,)), dma((NT,)),
        ],
        compiler_params=pltpu.CompilerParams(
            collective_id=0, has_side_effects=True, vmem_limit_bytes=65011712),
    )(x, w_gate, w_up, w_down)


def solution(mesh):
    return jax.shard_map(
        mlp,
        mesh=mesh,
        in_specs=(P("dp", None), P(None, "tp"), P(None, "tp"), P("tp", None)),
        out_specs=P("dp", None),
        check_vma=False,
    )
```

```python
import jax
import jax.numpy as jnp
from jax import lax
from jax.experimental import pallas as pl
from jax.experimental.pallas import tpu as pltpu
from jax.sharding import PartitionSpec as P

MESH = pl.DeviceIdType.MESH
F32 = jnp.float32
BF16 = jnp.bfloat16
ROWS = 128
HALF = ROWS // 2
D = 4096
F = 4096
FH = F // 2
KC = 512
NK = D // KC
XC = 256
NR = 6
NC = 4
NB = 256
DB = 512
ND = D // DB
XP = 16
WIDTHS = (256, 256, 512, 512, 512, 512, 512, 512, 256, 128, 128)
NT = len(WIDTHS)
OFFS = tuple(sum(WIDTHS[:j]) for j in range(NT))

SCHEDULE = (
    ('s',0,0), ('s',0,1), ('s',1,0), ('y',0), ('s',1,1), ('y',1), ('s',2,0), ('s',2,1), ('y',2), ('s',3,0),
    ('y',3), ('o','y0'), ('y',4), ('s',3,1), ('y',5), ('x',0), ('s',4,0), ('x',1), ('o','y1'), ('y',6),
    ('s',4,1), ('y',7), ('x',2), ('o','y2'), ('x',3), ('y',8), ('o','x0'), ('y',9), ('x',4), ('o','c0'),
    ('x',5), ('o','x1'), ('o','c1'), ('o','x2'), ('t',0), ('t',1), ('t',2), ('s',5,0), ('s',5,1), ('e',0),
    ('s',6,0), ('e',1), ('t',3), ('s',6,1), ('e',2), ('s',7,0), ('s',7,1), ('t',4), ('S',0), ('e',3), ('S',1),
    ('S',2), ('t',5), ('e',4), ('c',0), ('S',3), ('c',1), ('S',4), ('t',6), ('e',5), ('c',2), ('t',7), ('t',8),
    ('c',3), ('e',6), ('S',5), ('S',6), ('t',9), ('f',0), ('f',1), ('c',4), ('e',7), ('c',5), ('e',8), ('S',7),
    ('t',10), ('S',8), ('c',6), ('e',9), ('S',9), ('f',2), ('e',10), ('f',3), ('c',7), ('f',4), ('c',8),
    ('S',10), ('c',9), ('c',10), ('f',5), ('f',6), ('f',7), ('f',8), ('f',9), ('f',10),
)


def kernel(x_hbm, wg_hbm, wu_hbm, wd_hbm, y_ref,
           xs, xo, wg, wu, wd, acc_s, acc_o, h_s, h_o,
           tb_o, rb_o, uy, yr, tb_s, rb_s, ux, xr,
           f_sem, x_sem, g_sem, u_sem, w_sem,
           yx_send, yx_recv, xx_send, xx_recv, dx_send, dx_recv,
           do_send, do_recv, uy_send, uy_recv, ds_send, ds_recv,
           ux_send, ux_recv, gy_send, gy_recv):
    grp = lax.axis_index("dp")
    tp = lax.axis_index("tp")
    core = lax.rem(tp, 2)
    chip = tp // 2
    partner = {"tp": 2 * chip + (1 - core)}
    xpeer = {"tp": 2 * (1 - chip) + core}
    ypeer = {"dp": 1 - grp}
    mine = pl.ds(pl.multiple_of(core * HALF, HALF), HALF)
    theirs = pl.ds(pl.multiple_of((1 - core) * HALF, HALF), HALF)
    units = pl.ds(pl.multiple_of(grp * FH, FH), FH)

    def fence():
        pl.semaphore_signal(f_sem, 1)
        pl.semaphore_wait(f_sem, 1)

    barrier = pltpu.get_barrier_semaphore()
    for peer in (partner, xpeer, ypeer):
        pl.semaphore_signal(barrier, inc=1, device_id=peer, device_id_type=MESH)

    for p in range(0, HALF, XP):
        rows = pl.ds(pl.multiple_of(core * HALF + p, XP), XP)
        pltpu.make_async_copy(x_hbm.at[rows], xs.at[rows], x_sem.at[0]).start()
    x_mine = pltpu.make_async_copy(x_hbm.at[mine], xs.at[mine], x_sem.at[0])
    x_theirs = pltpu.make_async_copy(x_hbm.at[theirs], xs.at[theirs], x_sem.at[1])

    def w_copies(k):
        rows = pl.ds(k * KC, KC)
        return (pltpu.make_async_copy(wg_hbm.at[rows, units], wg.at[k], g_sem.at[k]),
                pltpu.make_async_copy(wu_hbm.at[rows, units], wu.at[k], u_sem.at[k]))

    def wd_copy(j):
        return pltpu.make_async_copy(wd_hbm.at[units, pl.ds(j * DB, DB)], wd.at[j], w_sem.at[j])

    def push(src, dst, send, recv, peer):
        return pltpu.make_async_remote_copy(src, dst, send, recv, device_id=peer, device_id_type=MESH)

    def relay_k(i, c):
        return 2 * (i // 2) + c

    def relay_cols(i, c):
        return pl.ds(pl.multiple_of(relay_k(i, c) * KC + (i % 2) * XC, XC), XC)

    def y_cols(i):
        if i < NR:
            return relay_cols(i, chip)
        return pl.ds(2 * NR * XC + (i - NR) * XC, XC)

    def y_x(i):
        c = y_cols(i)
        return push(xs.at[mine, c], xo.at[mine, c], yx_send.at[i], yx_recv.at[i], ypeer)

    def x_x(i, c):
        c = relay_cols(i, c)
        return push(xo.at[mine, c], xo.at[mine, c], xx_send.at[i], xx_recv.at[i], xpeer)

    def d_x(i):
        c = y_cols(i) if i < NR + NC else relay_cols(i - NR - NC, 1 - chip)
        return push(xo.at[mine, c], xo.at[mine, c], dx_send.at[i], dx_recv.at[i], partner)

    def on_y(i):
        y_x(i).wait_recv()
        if i < NR:
            x_x(i, chip).start()
        d_x(i).start()

    def on_x(i):
        x_x(i, 1 - chip).wait_recv()
        d_x(NR + NC + i).start()

    waited = set()

    def wait_w(*ks):
        for k in ks:
            if k not in waited:
                waited.add(k)
                for c in w_copies(k):
                    c.wait()

    def wait_wd(j):
        if ("d", j) not in waited:
            waited.add(("d", j))
            wd_copy(j).wait()

    def gate_up(xref, acc, k, lo, hi, first, h):
        cols = pl.ds(k * KC if isinstance(k, int) else pl.multiple_of(k * KC, KC), KC)
        for n in range(lo, hi, NB):
            nn = pl.ds(n, NB)
            g = jnp.dot(xref[:, cols], wg[k, :, nn], preferred_element_type=F32)
            u = jnp.dot(xref[:, cols], wu[k, :, nn], preferred_element_type=F32)
            if not first:
                g = acc[0, :, nn] + g
                u = acc[1, :, nn] + u
            if h is None:
                acc[0, :, nn] = g
                acc[1, :, nn] = u
            else:
                h[:, nn] = (jax.nn.silu(g) * u).astype(BF16)

    def own(k, half):
        wait_w(k)
        if "x" not in waited:
            waited.add("x")
            x_theirs.wait()
        lo = half * (FH // 2)
        gate_up(xs, acc_s, k, lo, lo + FH // 2, k == 0, h_s if k == NK - 1 else None)

    slots = [t[1] for t in SCHEDULE if t[0] == "o"]

    def other(slot):
        kind, r = slot[0], int(slot[1])
        if kind == "c":
            wait_w(NR + r)
            k = NR + r
            ready = (NR + 2 * r, NR + 2 * r + 1)
        else:
            wait_w(2 * r, 2 * r + 1)
            k = relay_k(2 * r, chip if kind == "y" else 1 - chip)
            base = 0 if kind == "y" else NR + NC
            ready = (base + 2 * r, base + 2 * r + 1)
        for i in ready:
            d_x(i).wait_recv()
        gate_up(xo, acc_o, k, 0, FH, slot == slots[0], h_o if slot == slots[-1] else None)

    def block(j):
        return pl.ds(OFFS[j], WIDTHS[j])

    def term(h, acc, tb, j):
        o, w = OFFS[j], WIDTHS[j]
        wait_wd(o // DB)
        acc[o // FH, :, pl.ds(o % FH, w)] = jnp.dot(
            h[...], wd[o // DB, :, pl.ds(o % DB, w)], preferred_element_type=F32)
        tb[:, block(j)] = acc[o // FH, theirs, pl.ds(o % FH, w)].astype(BF16)

    def part(acc, j):
        o, w = OFFS[j], WIDTHS[j]
        return acc[o // FH, mine, pl.ds(o % FH, w)]

    def core_o(j):
        return push(tb_o.at[:, block(j)], rb_o.at[:, block(j)], do_send.at[j], do_recv.at[j], partner)

    def core_s(j):
        return push(tb_s.at[:, block(j)], rb_s.at[:, block(j)], ds_send.at[j], ds_recv.at[j], partner)

    def over_y(j):
        return push(uy.at[:, block(j)], yr.at[:, block(j)], uy_send.at[j], uy_recv.at[j], ypeer)

    def over_x(j):
        return push(ux.at[:, block(j)], xr.at[:, block(j)], ux_send.at[j], ux_recv.at[j], xpeer)

    def gather(j):
        rows = y_ref.at[mine, block(j)]
        return push(rows, rows, gy_send.at[j], gy_recv.at[j], partner)

    def send_y(j):
        core_o(j).wait_recv()
        uy[:, block(j)] = (part(acc_o, j) + rb_o[:, block(j)].astype(F32)).astype(BF16)
        over_y(j).start()

    def send_x(j):
        core_s(j).wait_recv()
        over_y(j).wait_recv()
        ux[:, block(j)] = (part(acc_s, j) + rb_s[:, block(j)].astype(F32)
                           + yr[:, block(j)].astype(F32)).astype(BF16)
        over_x(j).start()

    def finish(j):
        over_x(j).wait_recv()
        y_ref[mine, block(j)] = (ux[:, block(j)].astype(F32) + xr[:, block(j)].astype(F32)).astype(BF16)
        gather(j).start()

    fence()
    for k in range(NK):
        for c in w_copies(k):
            c.start()
        if k == 0:
            fence()
            x_theirs.start()
        fence()
    for j in range(ND):
        wd_copy(j).start()
    pl.semaphore_wait(barrier, 3)
    x_mine.wait()
    for i in range(NR + NC):
        y_x(i).start()

    for kind, i, *rest in SCHEDULE:
        if kind == "y":
            on_y(i)
        elif kind == "x":
            on_x(i)
        elif kind == "s":
            own(i, *rest)
        elif kind == "o":
            other(i, *rest)
        elif kind == "t":
            term(h_o, acc_o, tb_o, i, *rest)
            core_o(i).start()
        elif kind == "S":
            term(h_s, acc_s, tb_s, i, *rest)
            core_s(i).start()
        elif kind == "e":
            send_y(i)
        elif kind == "c":
            send_x(i)
        else:
            finish(i)

    for j in range(NT):
        gather(j).wait_recv()
    for i in range(NR + NC):
        y_x(i).wait_send()
        d_x(i).wait_send()
    for i in range(NR):
        x_x(i, chip).wait_send()
        d_x(NR + NC + i).wait_send()
    for j in range(NT):
        core_o(j).wait_send()
        core_s(j).wait_send()
        over_y(j).wait_send()
        over_x(j).wait_send()
        gather(j).wait_send()


def mlp(x, w_gate, w_up, w_down):
    dma = pltpu.SemaphoreType.DMA
    half = pltpu.VMEM((HALF, D), BF16)
    return pl.pallas_call(
        kernel,
        name="mlp",
        out_shape=pltpu.VMEM((ROWS, D), BF16),
        in_specs=[pl.BlockSpec(memory_space=pl.ANY)] * 4,
        out_specs=pl.BlockSpec(memory_space=pltpu.VMEM),
        scratch_shapes=[
            pltpu.VMEM((ROWS, D), BF16),
            pltpu.VMEM((ROWS, D), BF16),
            pltpu.VMEM((NK, KC, FH), BF16),
            pltpu.VMEM((NK, KC, FH), BF16),
            pltpu.VMEM((ND, FH, DB), BF16),
            pltpu.VMEM((2, ROWS, FH), F32),
            pltpu.VMEM((2, ROWS, FH), F32),
            pltpu.VMEM((ROWS, FH), BF16),
            pltpu.VMEM((ROWS, FH), BF16),
            half, half, half, half, half, half, half, half,
            pltpu.SemaphoreType.REGULAR,
            dma((2,)), dma((NK,)), dma((NK,)), dma((ND,)),
            dma((NR + NC,)), dma((NR + NC,)), dma((NR,)), dma((NR,)),
            dma((2 * NR + NC,)), dma((2 * NR + NC,)),
            dma((NT,)), dma((NT,)), dma((NT,)), dma((NT,)), dma((NT,)), dma((NT,)),
            dma((NT,)), dma((NT,)), dma((NT,)), dma((NT,)),
        ],
        compiler_params=pltpu.CompilerParams(
            collective_id=0, has_side_effects=True, vmem_limit_bytes=65011712),
    )(x, w_gate, w_up, w_down)


def solution(mesh):
    return jax.shard_map(
        mlp,
        mesh=mesh,
        in_specs=(P("dp", None), P(None, "tp"), P(None, "tp"), P("tp", None)),
        out_specs=P("dp", None),
        check_vma=False,
    )
```

```python
import jax
import jax.numpy as jnp
from jax import lax
from jax.experimental import pallas as pl
from jax.experimental.pallas import tpu as pltpu
from jax.sharding import PartitionSpec as P

MESH = pl.DeviceIdType.MESH
F32 = jnp.float32
BF16 = jnp.bfloat16
ROWS = 128
HALF = ROWS // 2
D = 4096
F = 4096
FH = F // 2
KC = 512
NK = D // KC
XC = 256
NR = 6
NC = 4
NB = 256
DB = 512
ND = D // DB
XP = 16
WIDTHS = (256, 256, 256, 256, 256, 256, 256, 256, 256, 256, 256, 256, 256, 256, 128, 128, 128, 128)
NT = len(WIDTHS)
OFFS = tuple(sum(WIDTHS[:j]) for j in range(NT))

SCHEDULE = (
    ('s',0,2), ('y',0), ('s',1,2), ('y',1), ('s',2,2), ('y',2), ('y',3), ('s',3,2), ('y',4), ('o','y0'),
    ('y',5), ('x',0), ('o','y1'), ('x',1), ('y',6), ('s',4,2), ('y',7), ('x',2), ('o','y2'), ('x',3), ('y',8),
    ('o','x0'), ('y',9), ('x',4), ('o','c0'), ('x',5), ('o','x1'), ('o','c1'), ('o','x2'), ('t',0), ('t',1),
    ('t',2), ('t',3), ('s',5,2), ('e',0), ('t',4), ('e',1), ('s',6,2), ('e',2), ('e',3), ('s',7,2), ('t',5),
    ('S',0), ('S',1), ('e',4), ('t',6), ('t',7), ('t',8), ('S',2), ('c',0), ('e',5), ('t',9), ('S',3), ('c',1),
    ('e',6), ('e',7), ('t',10), ('S',4), ('c',2), ('e',8), ('S',5), ('t',11), ('c',3), ('S',6), ('t',12),
    ('e',9), ('c',4), ('e',10), ('S',7), ('t',13), ('c',5), ('e',11), ('t',14), ('f',0), ('S',8), ('c',6),
    ('t',15), ('S',9), ('e',12), ('c',7), ('S',10), ('S',11), ('e',13), ('e',14), ('c',8), ('f',1), ('t',16),
    ('f',2), ('S',12), ('e',15), ('c',9), ('t',17), ('S',13), ('S',14), ('c',10), ('f',3), ('e',16), ('S',15),
    ('f',4), ('c',11), ('e',17), ('S',16), ('S',17), ('c',12), ('c',13), ('c',14), ('c',15), ('c',16), ('f',5),
    ('f',6), ('f',7), ('c',17), ('f',8), ('f',9), ('f',10), ('f',11), ('f',12), ('f',13), ('f',14), ('f',15),
    ('f',16), ('f',17),
)


def kernel(x_hbm, wg_hbm, wu_hbm, wd_hbm, y_ref,
           xs, xo, wg, wu, wd, acc_s, acc_o, h_s, h_o,
           tb_o, rb_o, uy, yr, tb_s, rb_s, ux, xr,
           f_sem, x_sem, g_sem, u_sem, w_sem,
           yx_send, yx_recv, xx_send, xx_recv, dx_send, dx_recv,
           do_send, do_recv, uy_send, uy_recv, ds_send, ds_recv,
           ux_send, ux_recv, gy_send, gy_recv):
    grp = lax.axis_index("dp")
    tp = lax.axis_index("tp")
    core = lax.rem(tp, 2)
    chip = tp // 2
    partner = {"tp": 2 * chip + (1 - core)}
    xpeer = {"tp": 2 * (1 - chip) + core}
    ypeer = {"dp": 1 - grp}
    mine = pl.ds(pl.multiple_of(core * HALF, HALF), HALF)
    theirs = pl.ds(pl.multiple_of((1 - core) * HALF, HALF), HALF)
    units = pl.ds(pl.multiple_of(grp * FH, FH), FH)

    def fence():
        pl.semaphore_signal(f_sem, 1)
        pl.semaphore_wait(f_sem, 1)

    barrier = pltpu.get_barrier_semaphore()
    for peer in (partner, xpeer, ypeer):
        pl.semaphore_signal(barrier, inc=1, device_id=peer, device_id_type=MESH)

    for p in range(0, HALF, XP):
        rows = pl.ds(pl.multiple_of(core * HALF + p, XP), XP)
        pltpu.make_async_copy(x_hbm.at[rows], xs.at[rows], x_sem.at[0]).start()
    x_mine = pltpu.make_async_copy(x_hbm.at[mine], xs.at[mine], x_sem.at[0])
    x_theirs = pltpu.make_async_copy(x_hbm.at[theirs], xs.at[theirs], x_sem.at[1])

    def w_copies(k):
        rows = pl.ds(k * KC, KC)
        return (pltpu.make_async_copy(wg_hbm.at[rows, units], wg.at[k], g_sem.at[k]),
                pltpu.make_async_copy(wu_hbm.at[rows, units], wu.at[k], u_sem.at[k]))

    def wd_copy(j):
        return pltpu.make_async_copy(wd_hbm.at[units, pl.ds(j * DB, DB)], wd.at[j], w_sem.at[j])

    def push(src, dst, send, recv, peer):
        return pltpu.make_async_remote_copy(src, dst, send, recv, device_id=peer, device_id_type=MESH)

    def relay_k(i, c):
        return 2 * (i // 2) + c

    def relay_cols(i, c):
        return pl.ds(pl.multiple_of(relay_k(i, c) * KC + (i % 2) * XC, XC), XC)

    def y_cols(i):
        if i < NR:
            return relay_cols(i, chip)
        return pl.ds(2 * NR * XC + (i - NR) * XC, XC)

    def y_x(i):
        c = y_cols(i)
        return push(xs.at[mine, c], xo.at[mine, c], yx_send.at[i], yx_recv.at[i], ypeer)

    def x_x(i, c):
        c = relay_cols(i, c)
        return push(xo.at[mine, c], xo.at[mine, c], xx_send.at[i], xx_recv.at[i], xpeer)

    def d_x(i):
        c = y_cols(i) if i < NR + NC else relay_cols(i - NR - NC, 1 - chip)
        return push(xo.at[mine, c], xo.at[mine, c], dx_send.at[i], dx_recv.at[i], partner)

    def on_y(i):
        y_x(i).wait_recv()
        if i < NR:
            x_x(i, chip).start()
        d_x(i).start()

    def on_x(i):
        x_x(i, 1 - chip).wait_recv()
        d_x(NR + NC + i).start()

    waited = set()

    def wait_w(*ks):
        for k in ks:
            if k not in waited:
                waited.add(k)
                for c in w_copies(k):
                    c.wait()

    def wait_wd(j):
        if ("d", j) not in waited:
            waited.add(("d", j))
            wd_copy(j).wait()

    def gate_up(xref, acc, k, lo, hi, first, h):
        cols = pl.ds(k * KC if isinstance(k, int) else pl.multiple_of(k * KC, KC), KC)
        for n in range(lo, hi, NB):
            nn = pl.ds(n, NB)
            g = jnp.dot(xref[:, cols], wg[k, :, nn], preferred_element_type=F32)
            u = jnp.dot(xref[:, cols], wu[k, :, nn], preferred_element_type=F32)
            if not first:
                g = acc[0, :, nn] + g
                u = acc[1, :, nn] + u
            if h is None:
                acc[0, :, nn] = g
                acc[1, :, nn] = u
            else:
                h[:, nn] = (jax.nn.silu(g) * u).astype(BF16)

    def own(k, half):
        wait_w(k)
        if "x" not in waited:
            waited.add("x")
            x_theirs.wait()
        lo, hi = (0, FH) if half == 2 else (half * (FH // 2), (half + 1) * (FH // 2))
        gate_up(xs, acc_s, k, lo, hi, k == 0, h_s if k == NK - 1 else None)

    slots = [t[1] for t in SCHEDULE if t[0] == "o"]

    def other(slot):
        kind, r = slot[0], int(slot[1])
        if kind == "c":
            wait_w(NR + r)
            k = NR + r
            ready = (NR + 2 * r, NR + 2 * r + 1)
        else:
            wait_w(2 * r, 2 * r + 1)
            k = relay_k(2 * r, chip if kind == "y" else 1 - chip)
            base = 0 if kind == "y" else NR + NC
            ready = (base + 2 * r, base + 2 * r + 1)
        for i in ready:
            d_x(i).wait_recv()
        gate_up(xo, acc_o, k, 0, FH, slot == slots[0], h_o if slot == slots[-1] else None)

    def block(j):
        return pl.ds(OFFS[j], WIDTHS[j])

    def term(h, acc, tb, j):
        o, w = OFFS[j], WIDTHS[j]
        wait_wd(o // DB)
        acc[o // FH, :, pl.ds(o % FH, w)] = jnp.dot(
            h[...], wd[o // DB, :, pl.ds(o % DB, w)], preferred_element_type=F32)
        tb[:, block(j)] = acc[o // FH, theirs, pl.ds(o % FH, w)].astype(BF16)

    def part(acc, j):
        o, w = OFFS[j], WIDTHS[j]
        return acc[o // FH, mine, pl.ds(o % FH, w)]

    def core_o(j):
        return push(tb_o.at[:, block(j)], rb_o.at[:, block(j)], do_send.at[j], do_recv.at[j], partner)

    def core_s(j):
        return push(tb_s.at[:, block(j)], rb_s.at[:, block(j)], ds_send.at[j], ds_recv.at[j], partner)

    def over_y(j):
        return push(uy.at[:, block(j)], yr.at[:, block(j)], uy_send.at[j], uy_recv.at[j], ypeer)

    def over_x(j):
        return push(ux.at[:, block(j)], xr.at[:, block(j)], ux_send.at[j], ux_recv.at[j], xpeer)

    def gather(j):
        rows = y_ref.at[mine, block(j)]
        return push(rows, rows, gy_send.at[j], gy_recv.at[j], partner)

    def send_y(j):
        core_o(j).wait_recv()
        uy[:, block(j)] = (part(acc_o, j) + rb_o[:, block(j)].astype(F32)).astype(BF16)
        over_y(j).start()

    def send_x(j):
        core_s(j).wait_recv()
        over_y(j).wait_recv()
        ux[:, block(j)] = (part(acc_s, j) + rb_s[:, block(j)].astype(F32)
                           + yr[:, block(j)].astype(F32)).astype(BF16)
        over_x(j).start()

    def finish(j):
        over_x(j).wait_recv()
        y_ref[mine, block(j)] = (ux[:, block(j)].astype(F32) + xr[:, block(j)].astype(F32)).astype(BF16)
        gather(j).start()

    fence()
    for k in range(NK):
        for c in w_copies(k):
            c.start()
        if k == 0:
            fence()
            x_theirs.start()
        fence()
    for j in range(ND):
        wd_copy(j).start()
    pl.semaphore_wait(barrier, 3)
    x_mine.wait()
    for i in range(NR + NC):
        y_x(i).start()

    for kind, i, *rest in SCHEDULE:
        if kind == "y":
            on_y(i)
        elif kind == "x":
            on_x(i)
        elif kind == "s":
            own(i, *rest)
        elif kind == "o":
            other(i, *rest)
        elif kind == "t":
            term(h_o, acc_o, tb_o, i, *rest)
            core_o(i).start()
        elif kind == "S":
            term(h_s, acc_s, tb_s, i, *rest)
            core_s(i).start()
        elif kind == "e":
            send_y(i)
        elif kind == "c":
            send_x(i)
        else:
            finish(i)

    for j in range(NT):
        gather(j).wait_recv()
    for i in range(NR + NC):
        y_x(i).wait_send()
        d_x(i).wait_send()
    for i in range(NR):
        x_x(i, chip).wait_send()
        d_x(NR + NC + i).wait_send()
    for j in range(NT):
        core_o(j).wait_send()
        core_s(j).wait_send()
        over_y(j).wait_send()
        over_x(j).wait_send()
        gather(j).wait_send()


def mlp(x, w_gate, w_up, w_down):
    dma = pltpu.SemaphoreType.DMA
    half = pltpu.VMEM((HALF, D), BF16)
    return pl.pallas_call(
        kernel,
        name="mlp",
        out_shape=pltpu.VMEM((ROWS, D), BF16),
        in_specs=[pl.BlockSpec(memory_space=pl.ANY)] * 4,
        out_specs=pl.BlockSpec(memory_space=pltpu.VMEM),
        scratch_shapes=[
            pltpu.VMEM((ROWS, D), BF16),
            pltpu.VMEM((ROWS, D), BF16),
            pltpu.VMEM((NK, KC, FH), BF16),
            pltpu.VMEM((NK, KC, FH), BF16),
            pltpu.VMEM((ND, FH, DB), BF16),
            pltpu.VMEM((2, ROWS, FH), F32),
            pltpu.VMEM((2, ROWS, FH), F32),
            pltpu.VMEM((ROWS, FH), BF16),
            pltpu.VMEM((ROWS, FH), BF16),
            half, half, half, half, half, half, half, half,
            pltpu.SemaphoreType.REGULAR,
            dma((2,)), dma((NK,)), dma((NK,)), dma((ND,)),
            dma((NR + NC,)), dma((NR + NC,)), dma((NR,)), dma((NR,)),
            dma((2 * NR + NC,)), dma((2 * NR + NC,)),
            dma((NT,)), dma((NT,)), dma((NT,)), dma((NT,)), dma((NT,)), dma((NT,)),
            dma((NT,)), dma((NT,)), dma((NT,)), dma((NT,)),
        ],
        compiler_params=pltpu.CompilerParams(
            collective_id=0, has_side_effects=True, vmem_limit_bytes=65011712),
    )(x, w_gate, w_up, w_down)


def solution(mesh):
    return jax.shard_map(
        mlp,
        mesh=mesh,
        in_specs=(P("dp", None), P(None, "tp"), P(None, "tp"), P("tp", None)),
        out_specs=P("dp", None),
        check_vma=False,
    )
```

```python
import jax
import jax.numpy as jnp
from jax import lax
from jax.experimental import pallas as pl
from jax.experimental.pallas import tpu as pltpu
from jax.sharding import PartitionSpec as P

MESH = pl.DeviceIdType.MESH
F32 = jnp.float32
BF16 = jnp.bfloat16
ROWS = 128
HALF = ROWS // 2
D = 4096
F = 4096
FH = F // 2
KC = 512
NK = D // KC
XC = 256
NR = 6
NC = 4
NB = 256
DB = 512
TU = 128
ND = D // DB
NX = D // XC
WIDTHS = (256, 256, 512, 512, 512, 512, 512, 512, 256, 128, 128)
NT = len(WIDTHS)
OFFS = tuple(sum(WIDTHS[:j]) for j in range(NT))

SCHEDULE = (
    ('s',0,0), ('s',0,1), ('s',1,0), ('y',0), ('s',1,1), ('y',1), ('s',2,0), ('s',2,1), ('y',2), ('s',3,0),
    ('y',3), ('o','y0'), ('y',4), ('s',3,1), ('y',5), ('x',0), ('s',4,0), ('x',1), ('o','y1'), ('y',6),
    ('s',4,1), ('y',7), ('x',2), ('o','y2'), ('x',3), ('y',8), ('o','x0'), ('y',9), ('x',4), ('o','c0'),
    ('x',5), ('o','x1'), ('o','c1'), ('o','x2'), ('t',0), ('t',1), ('t',2), ('s',5,0), ('s',5,1), ('e',0),
    ('s',6,0), ('e',1), ('t',3), ('s',6,1), ('e',2), ('s',7,0), ('s',7,1), ('t',4), ('S',0), ('e',3), ('S',1),
    ('S',2), ('t',5), ('e',4), ('c',0), ('S',3), ('c',1), ('S',4), ('t',6), ('e',5), ('c',2), ('t',7), ('t',8),
    ('c',3), ('e',6), ('S',5), ('S',6), ('t',9), ('f',0), ('f',1), ('c',4), ('e',7), ('c',5), ('e',8), ('S',7),
    ('t',10), ('S',8), ('c',6), ('e',9), ('S',9), ('f',2), ('e',10), ('f',3), ('c',7), ('f',4), ('c',8),
    ('S',10), ('c',9), ('c',10), ('f',5), ('f',6), ('f',7), ('f',8), ('f',9), ('f',10),
)


def kernel(x_hbm, wg_hbm, wu_hbm, wd_hbm, y_ref,
           xs, xo, wg, wu, wd, acc_s, acc_o, h_s, h_o,
           tb_o, rb_o, uy, yr, tb_s, rb_s, ux, xr,
           f_sem, x_sem, g_sem, u_sem, w_sem,
           yx_send, yx_recv, xx_send, xx_recv, dx_send, dx_recv,
           do_send, do_recv, uy_send, uy_recv, ds_send, ds_recv,
           ux_send, ux_recv, gy_send, gy_recv):
    grp = lax.axis_index("dp")
    tp = lax.axis_index("tp")
    core = lax.rem(tp, 2)
    chip = tp // 2
    partner = {"tp": 2 * chip + (1 - core)}
    xpeer = {"tp": 2 * (1 - chip) + core}
    ypeer = {"dp": 1 - grp}
    mine = pl.ds(pl.multiple_of(core * HALF, HALF), HALF)
    theirs = pl.ds(pl.multiple_of((1 - core) * HALF, HALF), HALF)
    units = pl.ds(pl.multiple_of(grp * FH, FH), FH)

    def fence():
        pl.semaphore_signal(f_sem, 1)
        pl.semaphore_wait(f_sem, 1)

    barrier = pltpu.get_barrier_semaphore()
    for peer in (partner, xpeer, ypeer):
        pl.semaphore_signal(barrier, inc=1, device_id=peer, device_id_type=MESH)

    def x_read(u, rows, q):
        cols = pl.ds(u * XC if isinstance(u, int) else pl.multiple_of(u * XC, XC), XC)
        return pltpu.make_async_copy(x_hbm.at[rows, cols], xs.at[u, rows], x_sem.at[q, u])


    def w_copies(k):
        rows = pl.ds(k * KC, KC)
        return (pltpu.make_async_copy(wg_hbm.at[rows, units], wg.at[k], g_sem.at[k]),
                pltpu.make_async_copy(wu_hbm.at[rows, units], wu.at[k], u_sem.at[k]))

    def wd_copy(j):
        return pltpu.make_async_copy(wd_hbm.at[units, pl.ds(j * DB, DB)], wd.at[j], w_sem.at[j])

    def push(src, dst, send, recv, peer):
        return pltpu.make_async_remote_copy(src, dst, send, recv, device_id=peer, device_id_type=MESH)

    def relay_k(i, c):
        return 2 * (i // 2) + c

    def relay_u(i, c):
        return 2 * relay_k(i, c) + i % 2

    def y_unit(i):
        return relay_u(i, chip) if i < NR else NR + i

    def y_x(i):
        u = y_unit(i)
        return push(xs.at[u, mine], xo.at[u, mine], yx_send.at[i], yx_recv.at[i], ypeer)

    def x_x(i, c):
        u = relay_u(i, c)
        return push(xo.at[u, mine], xo.at[u, mine], xx_send.at[i], xx_recv.at[i], xpeer)

    def d_x(i):
        u = y_unit(i) if i < NR + NC else relay_u(i - NR - NC, 1 - chip)
        return push(xo.at[u, mine], xo.at[u, mine], dx_send.at[i], dx_recv.at[i], partner)

    def on_y(i):
        y_x(i).wait_recv()
        if i < NR:
            x_x(i, chip).start()
        d_x(i).start()

    def on_x(i):
        x_x(i, 1 - chip).wait_recv()
        d_x(NR + NC + i).start()

    waited = set()

    def wait_w(*ks):
        for k in ks:
            if k not in waited:
                waited.add(k)
                for c in w_copies(k):
                    c.wait()

    def wait_wd(j):
        if ("d", j) not in waited:
            waited.add(("d", j))
            wd_copy(j).wait()

    def gate_up(xref, acc, k, lo, hi, first, h):
        lhs = jnp.concatenate([xref[2 * k], xref[2 * k + 1]], axis=1)
        for n in range(lo, hi, NB):
            nn = pl.ds(n, NB)
            g = jnp.dot(lhs, wg[k, :, nn], preferred_element_type=F32)
            u = jnp.dot(lhs, wu[k, :, nn], preferred_element_type=F32)
            if not first:
                g = acc[0, :, nn] + g
                u = acc[1, :, nn] + u
            if h is None:
                acc[0, :, nn] = g
                acc[1, :, nn] = u
            else:
                h[:, nn] = (jax.nn.silu(g) * u).astype(BF16)

    def own(k, half):
        wait_w(k)
        if "x" not in waited:
            waited.add("x")
            for i in range(NR):
                x_read(relay_u(i, 1 - chip), mine, 0).wait()
            for u in range(NX):
                x_read(u, theirs, 1).wait()
        lo, hi = (0, FH) if half == 2 else (half * (FH // 2), (half + 1) * (FH // 2))
        gate_up(xs, acc_s, k, lo, hi, k == 0, h_s if k == NK - 1 else None)

    slots = [t[1] for t in SCHEDULE if t[0] == "o"]

    def other(slot):
        kind, r = slot[0], int(slot[1])
        if kind == "c":
            wait_w(NR + r)
            k = NR + r
            ready = (NR + 2 * r, NR + 2 * r + 1)
        else:
            wait_w(2 * r, 2 * r + 1)
            k = relay_k(2 * r, chip if kind == "y" else 1 - chip)
            base = 0 if kind == "y" else NR + NC
            ready = (base + 2 * r, base + 2 * r + 1)
        for i in ready:
            d_x(i).wait_recv()
        gate_up(xo, acc_o, k, 0, FH, slot == slots[0], h_o if slot == slots[-1] else None)

    def block(j):
        return pl.ds(OFFS[j], WIDTHS[j])

    def units_of(j):
        return pl.ds(OFFS[j] // TU, WIDTHS[j] // TU)

    def lanes(j):
        for o in range(OFFS[j], OFFS[j] + WIDTHS[j], TU):
            yield o // TU, o // FH, pl.ds(o % FH, TU)

    def term(h, acc, tb, j):
        o, w = OFFS[j], WIDTHS[j]
        wait_wd(o // DB)
        acc[o // FH, :, pl.ds(o % FH, w)] = jnp.dot(
            h[...], wd[o // DB, :, pl.ds(o % DB, w)], preferred_element_type=F32)
        for u, q, cc in lanes(j):
            tb[u] = acc[q, theirs, cc].astype(BF16)

    def hop(src, dst, send, recv, j, peer):
        return push(src.at[units_of(j)], dst.at[units_of(j)], send.at[j], recv.at[j], peer)

    def core_o(j):
        return hop(tb_o, rb_o, do_send, do_recv, j, partner)

    def core_s(j):
        return hop(tb_s, rb_s, ds_send, ds_recv, j, partner)

    def over_y(j):
        return hop(uy, yr, uy_send, uy_recv, j, ypeer)

    def over_x(j):
        return hop(ux, xr, ux_send, ux_recv, j, xpeer)

    def gather(j):
        rows = y_ref.at[mine, block(j)]
        return push(rows, rows, gy_send.at[j], gy_recv.at[j], partner)

    def send_y(j):
        core_o(j).wait_recv()
        for u, q, cc in lanes(j):
            uy[u] = (acc_o[q, mine, cc] + rb_o[u].astype(F32)).astype(BF16)
        over_y(j).start()

    def send_x(j):
        core_s(j).wait_recv()
        over_y(j).wait_recv()
        for u, q, cc in lanes(j):
            ux[u] = (acc_s[q, mine, cc] + rb_s[u].astype(F32) + yr[u].astype(F32)).astype(BF16)
        over_x(j).start()

    def finish(j):
        over_x(j).wait_recv()
        for u, q, cc in lanes(j):
            y_ref[mine, pl.ds(u * TU, TU)] = (ux[u].astype(F32) + xr[u].astype(F32)).astype(BF16)
        gather(j).start()

    sent = tuple(y_unit(i) for i in range(NR + NC))
    for u in sent:
        x_read(u, mine, 0).start()
    fence()
    for k in range(NK):
        for c in w_copies(k):
            c.start()
        if k == 0:
            fence()
            for i in range(NR):
                x_read(relay_u(i, 1 - chip), mine, 0).start()
            for u in range(NX):
                x_read(u, theirs, 1).start()
        fence()
    for j in range(ND):
        wd_copy(j).start()
    pl.semaphore_wait(barrier, 3)
    for i, u in enumerate(sent):
        x_read(u, mine, 0).wait()
        y_x(i).start()

    for kind, i, *rest in SCHEDULE:
        if kind == "y":
            on_y(i)
        elif kind == "x":
            on_x(i)
        elif kind == "s":
            own(i, *rest)
        elif kind == "o":
            other(i, *rest)
        elif kind == "t":
            term(h_o, acc_o, tb_o, i, *rest)
            core_o(i).start()
        elif kind == "S":
            term(h_s, acc_s, tb_s, i, *rest)
            core_s(i).start()
        elif kind == "e":
            send_y(i)
        elif kind == "c":
            send_x(i)
        else:
            finish(i)

    for j in range(NT):
        gather(j).wait_recv()
    for i in range(NR + NC):
        y_x(i).wait_send()
        d_x(i).wait_send()
    for i in range(NR):
        x_x(i, chip).wait_send()
        d_x(NR + NC + i).wait_send()
    for j in range(NT):
        core_o(j).wait_send()
        core_s(j).wait_send()
        over_y(j).wait_send()
        over_x(j).wait_send()
        gather(j).wait_send()


def mlp(x, w_gate, w_up, w_down):
    dma = pltpu.SemaphoreType.DMA
    half = pltpu.VMEM((D // TU, HALF, TU), BF16)
    return pl.pallas_call(
        kernel,
        name="mlp",
        out_shape=pltpu.VMEM((ROWS, D), BF16),
        in_specs=[pl.BlockSpec(memory_space=pl.ANY)] * 4,
        out_specs=pl.BlockSpec(memory_space=pltpu.VMEM),
        scratch_shapes=[
            pltpu.VMEM((NX, ROWS, XC), BF16),
            pltpu.VMEM((NX, ROWS, XC), BF16),
            pltpu.VMEM((NK, KC, FH), BF16),
            pltpu.VMEM((NK, KC, FH), BF16),
            pltpu.VMEM((ND, FH, DB), BF16),
            pltpu.VMEM((2, ROWS, FH), F32),
            pltpu.VMEM((2, ROWS, FH), F32),
            pltpu.VMEM((ROWS, FH), BF16),
            pltpu.VMEM((ROWS, FH), BF16),
            half, half, half, half, half, half, half, half,
            pltpu.SemaphoreType.REGULAR,
            dma((2, NX)), dma((NK,)), dma((NK,)), dma((ND,)),
            dma((NR + NC,)), dma((NR + NC,)), dma((NR,)), dma((NR,)),
            dma((2 * NR + NC,)), dma((2 * NR + NC,)),
            dma((NT,)), dma((NT,)), dma((NT,)), dma((NT,)), dma((NT,)), dma((NT,)),
            dma((NT,)), dma((NT,)), dma((NT,)), dma((NT,)),
        ],
        compiler_params=pltpu.CompilerParams(
            collective_id=0, has_side_effects=True, vmem_limit_bytes=65011712),
    )(x, w_gate, w_up, w_down)


def solution(mesh):
    return jax.shard_map(
        mlp,
        mesh=mesh,
        in_specs=(P("dp", None), P(None, "tp"), P(None, "tp"), P("tp", None)),
        out_specs=P("dp", None),
        check_vma=False,
    )
```

```python
import jax
import jax.numpy as jnp
from jax import lax
from jax.experimental import pallas as pl
from jax.experimental.pallas import tpu as pltpu
from jax.sharding import PartitionSpec as P

MESH = pl.DeviceIdType.MESH
F32 = jnp.float32
BF16 = jnp.bfloat16
ROWS = 128
HALF = ROWS // 2
D = 4096
F = 4096
FH = F // 2
KC = 512
NK = D // KC
XC = 256
NR = 6
NC = 4
NB = 256
DB = 512
TU = 128
ND = D // DB
NX = D // XC
WIDTHS = (512, 512, 512, 512, 512, 512, 512, 512)
NT = len(WIDTHS)
OFFS = tuple(sum(WIDTHS[:j]) for j in range(NT))
OWN_W = (512, 512, 1024, 1024, 1024)
NS = len(OWN_W)
OWN_O = tuple(sum(OWN_W[:j]) for j in range(NS))
OUT_W = (1024, 1024, 1024, 512, 512)
NG = len(OUT_W)
OUT_O = tuple(sum(OUT_W[:j]) for j in range(NG))

SCHEDULE = (
    ('s',0,0), ('s',0,1), ('y',0), ('s',1,0), ('y',1), ('s',1,1), ('s',2,0), ('y',2), ('s',2,1), ('o','y0'),
    ('y',3), ('s',3,0), ('x',0), ('s',3,1), ('y',4), ('x',1), ('o','y1'), ('y',5), ('s',4,0), ('o','x0'),
    ('y',6), ('s',4,1), ('y',7), ('x',2), ('x',3), ('o','y2'), ('y',8), ('x',4), ('x',5), ('o','c0'), ('y',9),
    ('o','x1'), ('o','x2'), ('o','c1'), ('t',0), ('t',1), ('s',5,0), ('s',5,1), ('e',0), ('s',6,0), ('s',6,1),
    ('e',1), ('t',2), ('s',7,0), ('s',7,1), ('S',0), ('t',3), ('e',2), ('S',1), ('c',0), ('t',4), ('e',3),
    ('S',2), ('c',1), ('t',5), ('e',4), ('S',3), ('c',2), ('t',6), ('e',5), ('c',3), ('t',7), ('e',6), ('c',4),
    ('e',7), ('S',4), ('f',0), ('f',1), ('c',5), ('c',6), ('f',2), ('c',7), ('f',3), ('g',0), ('f',4), ('g',1),
    ('f',5), ('g',2), ('f',6), ('g',3), ('f',7), ('g',4),
)


def kernel(x_hbm, wg_hbm, wu_hbm, wd_hbm, y_ref,
           xs, xo, wg, wu, wd, acc_s, acc_o, h_s, h_o,
           tb_o, rb_o, uy, yr, tb_s, rb_s, ux, xr,
           f_sem, x_sem, g_sem, u_sem, w_sem,
           yx_send, yx_recv, xx_send, xx_recv, dx_send, dx_recv,
           do_send, do_recv, uy_send, uy_recv, ds_send, ds_recv,
           ux_send, ux_recv, gy_send, gy_recv):
    grp = lax.axis_index("dp")
    tp = lax.axis_index("tp")
    core = lax.rem(tp, 2)
    chip = tp // 2
    partner = {"tp": 2 * chip + (1 - core)}
    xpeer = {"tp": 2 * (1 - chip) + core}
    ypeer = {"dp": 1 - grp}
    mine = pl.ds(pl.multiple_of(core * HALF, HALF), HALF)
    theirs = pl.ds(pl.multiple_of((1 - core) * HALF, HALF), HALF)
    units = pl.ds(pl.multiple_of(grp * FH, FH), FH)

    def fence():
        pl.semaphore_signal(f_sem, 1)
        pl.semaphore_wait(f_sem, 1)

    barrier = pltpu.get_barrier_semaphore()
    for peer in (partner, xpeer, ypeer):
        pl.semaphore_signal(barrier, inc=1, device_id=peer, device_id_type=MESH)

    def x_read(u, rows, q):
        cols = pl.ds(u * XC if isinstance(u, int) else pl.multiple_of(u * XC, XC), XC)
        return pltpu.make_async_copy(x_hbm.at[rows, cols], xs.at[u, rows], x_sem.at[q, u])


    def w_copies(k):
        rows = pl.ds(k * KC, KC)
        return (pltpu.make_async_copy(wg_hbm.at[rows, units], wg.at[k], g_sem.at[k]),
                pltpu.make_async_copy(wu_hbm.at[rows, units], wu.at[k], u_sem.at[k]))

    def wd_copy(j):
        return pltpu.make_async_copy(wd_hbm.at[units, pl.ds(j * DB, DB)], wd.at[j], w_sem.at[j])

    def push(src, dst, send, recv, peer):
        return pltpu.make_async_remote_copy(src, dst, send, recv, device_id=peer, device_id_type=MESH)

    def relay_k(i, c):
        return 2 * (i // 2) + c

    def relay_u(i, c):
        return 2 * relay_k(i, c) + i % 2

    def y_unit(i):
        return relay_u(i, chip) if i < NR else NR + i

    def y_x(i):
        u = y_unit(i)
        return push(xs.at[u, mine], xo.at[u, mine], yx_send.at[i], yx_recv.at[i], ypeer)

    def x_x(i, c):
        u = relay_u(i, c)
        return push(xo.at[u, mine], xo.at[u, mine], xx_send.at[i], xx_recv.at[i], xpeer)

    def d_x(m):
        if 2 * m < NR + NC:
            u = y_unit(2 * m)
        else:
            u = relay_u(2 * m - NR - NC, 1 - chip)
        both = xo.at[pl.ds(u, 2), mine]
        return push(both, both, dx_send.at[m], dx_recv.at[m], partner)

    def on_y(i):
        y_x(i).wait_recv()
        if i < NR:
            x_x(i, chip).start()
        if i % 2:
            d_x(i // 2).start()

    def on_x(i):
        x_x(i, 1 - chip).wait_recv()
        if i % 2:
            d_x((NR + NC + i) // 2).start()

    waited = set()

    def wait_w(*ks):
        for k in ks:
            if k not in waited:
                waited.add(k)
                for c in w_copies(k):
                    c.wait()

    def wait_wd(j):
        if ("d", j) not in waited:
            waited.add(("d", j))
            wd_copy(j).wait()

    def gate_up(xref, acc, k, lo, hi, first, h):
        lhs = jnp.concatenate([xref[2 * k], xref[2 * k + 1]], axis=1)
        for n in range(lo, hi, NB):
            nn = pl.ds(n, NB)
            g = jnp.dot(lhs, wg[k, :, nn], preferred_element_type=F32)
            u = jnp.dot(lhs, wu[k, :, nn], preferred_element_type=F32)
            if not first:
                g = acc[0, :, nn] + g
                u = acc[1, :, nn] + u
            if h is None:
                acc[0, :, nn] = g
                acc[1, :, nn] = u
            else:
                h[:, nn] = (jax.nn.silu(g) * u).astype(BF16)

    def own(k, half):
        wait_w(k)
        if "x" not in waited:
            waited.add("x")
            for i in range(NR):
                x_read(relay_u(i, 1 - chip), mine, 0).wait()
            for u in range(NX):
                x_read(u, theirs, 1).wait()
        lo, hi = (0, FH) if half == 2 else (half * (FH // 2), (half + 1) * (FH // 2))
        gate_up(xs, acc_s, k, lo, hi, k == 0, h_s if k == NK - 1 else None)

    slots = [t[1] for t in SCHEDULE if t[0] == "o"]

    def other(slot):
        kind, r = slot[0], int(slot[1])
        if kind == "c":
            wait_w(NR + r)
            k = NR + r
            ready = NR // 2 + r
        else:
            wait_w(2 * r, 2 * r + 1)
            k = relay_k(2 * r, chip if kind == "y" else 1 - chip)
            ready = r if kind == "y" else (NR + NC) // 2 + r
        d_x(ready).wait_recv()
        gate_up(xo, acc_o, k, 0, FH, slot == slots[0], h_o if slot == slots[-1] else None)

    def lanes(o, w):
        for p in range(o, o + w, TU):
            yield p // TU, p // FH, pl.ds(p % FH, TU)

    def term(h, acc, tb, o, w):
        for p in range(o, o + w, DB):
            wait_wd(p // DB)
        for p in range(o, o + w, min(w, DB)):
            n = min(w, DB)
            acc[p // FH, :, pl.ds(p % FH, n)] = jnp.dot(
                h[...], wd[p // DB, :, pl.ds(p % DB, n)], preferred_element_type=F32)
        for u, q, cc in lanes(o, w):
            tb[u] = acc[q, theirs, cc].astype(BF16)

    def hop(src, dst, send, recv, j, o, w, peer):
        units = pl.ds(o // TU, w // TU)
        return push(src.at[units], dst.at[units], send.at[j], recv.at[j], peer)

    def core_o(j):
        return hop(tb_o, rb_o, do_send, do_recv, j, OFFS[j], WIDTHS[j], partner)

    def core_s(j):
        return hop(tb_s, rb_s, ds_send, ds_recv, j, OWN_O[j], OWN_W[j], partner)

    def over_y(j):
        return hop(uy, yr, uy_send, uy_recv, j, OFFS[j], WIDTHS[j], ypeer)

    def over_x(j):
        return hop(ux, xr, ux_send, ux_recv, j, OFFS[j], WIDTHS[j], xpeer)

    def gather(j):
        rows = y_ref.at[mine, pl.ds(OUT_O[j], OUT_W[j])]
        return push(rows, rows, gy_send.at[j], gy_recv.at[j], partner)

    def send_y(j):
        core_o(j).wait_recv()
        for u, q, cc in lanes(OFFS[j], WIDTHS[j]):
            uy[u] = (acc_o[q, mine, cc] + rb_o[u].astype(F32)).astype(BF16)
        over_y(j).start()

    def send_x(j):
        for m in range(NS):
            if OWN_O[m] < OFFS[j] + WIDTHS[j] and OWN_O[m] + OWN_W[m] > OFFS[j] and ("s", m) not in waited:
                waited.add(("s", m))
                core_s(m).wait_recv()
        over_y(j).wait_recv()
        for u, q, cc in lanes(OFFS[j], WIDTHS[j]):
            ux[u] = (acc_s[q, mine, cc] + rb_s[u].astype(F32) + yr[u].astype(F32)).astype(BF16)
        over_x(j).start()

    def finish(j):
        over_x(j).wait_recv()
        for u, q, cc in lanes(OFFS[j], WIDTHS[j]):
            y_ref[mine, pl.ds(u * TU, TU)] = (ux[u].astype(F32) + xr[u].astype(F32)).astype(BF16)

    sent = tuple(y_unit(i) for i in range(NR + NC))
    for u in sent:
        x_read(u, mine, 0).start()
    fence()
    for k in range(NK):
        for c in w_copies(k):
            c.start()
        if k == 0:
            fence()
            for i in range(NR):
                x_read(relay_u(i, 1 - chip), mine, 0).start()
            for u in range(NX):
                x_read(u, theirs, 1).start()
        fence()
    for j in range(ND):
        wd_copy(j).start()
    pl.semaphore_wait(barrier, 3)
    for i, u in enumerate(sent):
        x_read(u, mine, 0).wait()
        y_x(i).start()

    for kind, i, *rest in SCHEDULE:
        if kind == "y":
            on_y(i)
        elif kind == "x":
            on_x(i)
        elif kind == "s":
            own(i, *rest)
        elif kind == "o":
            other(i, *rest)
        elif kind == "t":
            term(h_o, acc_o, tb_o, OFFS[i], WIDTHS[i])
            core_o(i).start()
        elif kind == "S":
            term(h_s, acc_s, tb_s, OWN_O[i], OWN_W[i])
            core_s(i).start()
        elif kind == "e":
            send_y(i)
        elif kind == "c":
            send_x(i)
        elif kind == "f":
            finish(i)
        else:
            gather(i).start()

    for j in range(NG):
        gather(j).wait_recv()
    for i in range(NR + NC):
        y_x(i).wait_send()
    for i in range(NR):
        x_x(i, chip).wait_send()
    for m in range(NX // 2):
        d_x(m).wait_send()
    for j in range(NT):
        core_o(j).wait_send()
        over_y(j).wait_send()
        over_x(j).wait_send()
    for j in range(NS):
        core_s(j).wait_send()
    for j in range(NG):
        gather(j).wait_send()


def mlp(x, w_gate, w_up, w_down):
    dma = pltpu.SemaphoreType.DMA
    half = pltpu.VMEM((D // TU, HALF, TU), BF16)
    return pl.pallas_call(
        kernel,
        name="mlp",
        out_shape=pltpu.VMEM((ROWS, D), BF16),
        in_specs=[pl.BlockSpec(memory_space=pl.ANY)] * 4,
        out_specs=pl.BlockSpec(memory_space=pltpu.VMEM),
        scratch_shapes=[
            pltpu.VMEM((NX, ROWS, XC), BF16),
            pltpu.VMEM((NX, ROWS, XC), BF16),
            pltpu.VMEM((NK, KC, FH), BF16),
            pltpu.VMEM((NK, KC, FH), BF16),
            pltpu.VMEM((ND, FH, DB), BF16),
            pltpu.VMEM((2, ROWS, FH), F32),
            pltpu.VMEM((2, ROWS, FH), F32),
            pltpu.VMEM((ROWS, FH), BF16),
            pltpu.VMEM((ROWS, FH), BF16),
            half, half, half, half, half, half, half, half,
            pltpu.SemaphoreType.REGULAR,
            dma((2, NX)), dma((NK,)), dma((NK,)), dma((ND,)),
            dma((NR + NC,)), dma((NR + NC,)), dma((NR,)), dma((NR,)),
            dma((NX // 2,)), dma((NX // 2,)),
            dma((NT,)), dma((NT,)), dma((NT,)), dma((NT,)), dma((NS,)), dma((NS,)),
            dma((NT,)), dma((NT,)), dma((NG,)), dma((NG,)),
        ],
        compiler_params=pltpu.CompilerParams(
            collective_id=0, has_side_effects=True, vmem_limit_bytes=65011712),
    )(x, w_gate, w_up, w_down)


def solution(mesh):
    return jax.shard_map(
        mlp,
        mesh=mesh,
        in_specs=(P("dp", None), P(None, "tp"), P(None, "tp"), P("tp", None)),
        out_specs=P("dp", None),
        check_vma=False,
    )
```

```python
import jax
import jax.numpy as jnp
from jax import lax
from jax.experimental import pallas as pl
from jax.experimental.pallas import tpu as pltpu
from jax.sharding import PartitionSpec as P

MESH = pl.DeviceIdType.MESH
F32 = jnp.float32
BF16 = jnp.bfloat16
ROWS = 128
HALF = ROWS // 2
D = 4096
F = 4096
FH = F // 2
KC = 512
NK = D // KC
XC = 512
NR = 3
NC = 2
NB = 256
DB = 512
TU = 128
ND = D // DB
NX = D // XC
WIDTHS = (256, 256, 512, 512, 512, 512, 512, 512, 512)
NT = len(WIDTHS)
OFFS = tuple(sum(WIDTHS[:j]) for j in range(NT))
OWN_W = (512, 512, 1024, 1024, 1024)
NS = len(OWN_W)
OWN_O = tuple(sum(OWN_W[:j]) for j in range(NS))
OUT_W = (2048, 1024, 512, 512)
NG = len(OUT_W)
OUT_O = tuple(sum(OUT_W[:j]) for j in range(NG))

SCHEDULE = (
    ('s',0,2), ('s',1,2), ('y',0), ('s',2,2), ('o','y0'), ('y',1), ('s',3,2), ('y',2), ('s',4,2), ('x',0),
    ('o','y1'), ('y',3), ('o','y2'), ('x',1), ('o','x0'), ('y',4), ('o','c0'), ('x',2), ('o','x1'), ('o','c1'),
    ('o','x2'), ('t',0), ('t',1), ('s',5,2), ('t',2), ('e',0), ('t',3), ('e',1), ('s',6,2), ('e',2), ('s',7,2),
    ('S',0), ('e',3), ('t',4), ('S',1), ('t',5), ('c',0), ('c',1), ('e',4), ('S',2), ('c',2), ('e',5), ('t',6),
    ('S',3), ('c',3), ('t',7), ('e',6), ('t',8), ('c',4), ('e',7), ('c',5), ('e',8), ('S',4), ('f',0), ('f',1),
    ('f',2), ('c',6), ('c',7), ('f',3), ('f',4), ('f',5), ('g',0), ('c',8), ('f',6), ('g',1), ('f',7), ('g',2),
    ('f',8), ('g',3),
)


def kernel(x_hbm, wg_hbm, wu_hbm, wd_hbm, y_ref,
           xs, xo, wg, wu, wd, acc_s, acc_o, h_s, h_o,
           tb_o, rb_o, uy, yr, tb_s, rb_s, ux, xr,
           f_sem, x_sem, g_sem, u_sem, w_sem,
           yx_send, yx_recv, xx_send, xx_recv, dx_send, dx_recv,
           do_send, do_recv, uy_send, uy_recv, ds_send, ds_recv,
           ux_send, ux_recv, gy_send, gy_recv):
    grp = lax.axis_index("dp")
    tp = lax.axis_index("tp")
    core = lax.rem(tp, 2)
    chip = tp // 2
    partner = {"tp": 2 * chip + (1 - core)}
    xpeer = {"tp": 2 * (1 - chip) + core}
    ypeer = {"dp": 1 - grp}
    mine = pl.ds(pl.multiple_of(core * HALF, HALF), HALF)
    theirs = pl.ds(pl.multiple_of((1 - core) * HALF, HALF), HALF)
    units = pl.ds(pl.multiple_of(grp * FH, FH), FH)

    def fence():
        pl.semaphore_signal(f_sem, 1)
        pl.semaphore_wait(f_sem, 1)

    barrier = pltpu.get_barrier_semaphore()
    for peer in (partner, xpeer, ypeer):
        pl.semaphore_signal(barrier, inc=1, device_id=peer, device_id_type=MESH)

    def x_read(u, rows, q):
        cols = pl.ds(u * XC if isinstance(u, int) else pl.multiple_of(u * XC, XC), XC)
        return pltpu.make_async_copy(x_hbm.at[rows, cols], xs.at[u, rows], x_sem.at[q, u])


    def w_copies(k):
        rows = pl.ds(k * KC, KC)
        return (pltpu.make_async_copy(wg_hbm.at[rows, units], wg.at[k], g_sem.at[k]),
                pltpu.make_async_copy(wu_hbm.at[rows, units], wu.at[k], u_sem.at[k]))

    def wd_copy(j):
        return pltpu.make_async_copy(wd_hbm.at[units, pl.ds(j * DB, DB)], wd.at[j], w_sem.at[j])

    def push(src, dst, send, recv, peer):
        return pltpu.make_async_remote_copy(src, dst, send, recv, device_id=peer, device_id_type=MESH)

    def relay_k(i, c):
        return 2 * i + c

    def relay_u(i, c):
        return relay_k(i, c)

    def y_unit(i):
        return relay_u(i, chip) if i < NR else NR + i

    def y_x(i):
        u = y_unit(i)
        return push(xs.at[u, mine], xo.at[u, mine], yx_send.at[i], yx_recv.at[i], ypeer)

    def x_x(i, c):
        u = relay_u(i, c)
        return push(xo.at[u, mine], xo.at[u, mine], xx_send.at[i], xx_recv.at[i], xpeer)

    def d_x(m):
        u = y_unit(m) if m < NR + NC else relay_u(m - NR - NC, 1 - chip)
        return push(xo.at[u, mine], xo.at[u, mine], dx_send.at[m], dx_recv.at[m], partner)

    def on_y(i):
        y_x(i).wait_recv()
        if i < NR:
            x_x(i, chip).start()
        d_x(i).start()

    def on_x(i):
        x_x(i, 1 - chip).wait_recv()
        d_x(NR + NC + i).start()

    waited = set()

    def wait_w(*ks):
        for k in ks:
            if k not in waited:
                waited.add(k)
                for c in w_copies(k):
                    c.wait()

    def wait_wd(j):
        if ("d", j) not in waited:
            waited.add(("d", j))
            wd_copy(j).wait()

    def gate_up(xref, acc, k, lo, hi, first, h):
        lhs = xref[k]
        for n in range(lo, hi, NB):
            nn = pl.ds(n, NB)
            g = jnp.dot(lhs, wg[k, :, nn], preferred_element_type=F32)
            u = jnp.dot(lhs, wu[k, :, nn], preferred_element_type=F32)
            if not first:
                g = acc[0, :, nn] + g
                u = acc[1, :, nn] + u
            if h is None:
                acc[0, :, nn] = g
                acc[1, :, nn] = u
            else:
                h[:, nn] = (jax.nn.silu(g) * u).astype(BF16)

    def own(k, half):
        wait_w(k)
        if "x" not in waited:
            waited.add("x")
            for i in range(NR):
                x_read(relay_u(i, 1 - chip), mine, 0).wait()
            for u in range(NX):
                x_read(u, theirs, 1).wait()
        lo, hi = (0, FH) if half == 2 else (half * (FH // 2), (half + 1) * (FH // 2))
        gate_up(xs, acc_s, k, lo, hi, k == 0, h_s if k == NK - 1 else None)

    slots = [t[1] for t in SCHEDULE if t[0] == "o"]

    def other(slot):
        kind, r = slot[0], int(slot[1])
        if kind == "c":
            k, ready = 2 * NR + r, NR + r
            wait_w(k)
        else:
            wait_w(2 * r, 2 * r + 1)
            k = relay_k(r, chip if kind == "y" else 1 - chip)
            ready = r if kind == "y" else NR + NC + r
        d_x(ready).wait_recv()
        gate_up(xo, acc_o, k, 0, FH, slot == slots[0], h_o if slot == slots[-1] else None)

    def lanes(o, w):
        for p in range(o, o + w, TU):
            yield p // TU, p // FH, pl.ds(p % FH, TU)

    def term(h, acc, tb, o, w):
        for p in range(o, o + w, DB):
            wait_wd(p // DB)
        for p in range(o, o + w, min(w, DB)):
            n = min(w, DB)
            acc[p // FH, :, pl.ds(p % FH, n)] = jnp.dot(
                h[...], wd[p // DB, :, pl.ds(p % DB, n)], preferred_element_type=F32)
        for u, q, cc in lanes(o, w):
            tb[u] = acc[q, theirs, cc].astype(BF16)

    def hop(src, dst, send, recv, j, o, w, peer):
        units = pl.ds(o // TU, w // TU)
        return push(src.at[units], dst.at[units], send.at[j], recv.at[j], peer)

    def core_o(j):
        return hop(tb_o, rb_o, do_send, do_recv, j, OFFS[j], WIDTHS[j], partner)

    def core_s(j):
        return hop(tb_s, rb_s, ds_send, ds_recv, j, OWN_O[j], OWN_W[j], partner)

    def over_y(j):
        return hop(uy, yr, uy_send, uy_recv, j, OFFS[j], WIDTHS[j], ypeer)

    def over_x(j):
        return hop(ux, xr, ux_send, ux_recv, j, OFFS[j], WIDTHS[j], xpeer)

    def gather(j):
        rows = y_ref.at[mine, pl.ds(OUT_O[j], OUT_W[j])]
        return push(rows, rows, gy_send.at[j], gy_recv.at[j], partner)

    def send_y(j):
        core_o(j).wait_recv()
        for u, q, cc in lanes(OFFS[j], WIDTHS[j]):
            uy[u] = (acc_o[q, mine, cc] + rb_o[u].astype(F32)).astype(BF16)
        over_y(j).start()

    def send_x(j):
        for m in range(NS):
            if OWN_O[m] < OFFS[j] + WIDTHS[j] and OWN_O[m] + OWN_W[m] > OFFS[j] and ("s", m) not in waited:
                waited.add(("s", m))
                core_s(m).wait_recv()
        over_y(j).wait_recv()
        for u, q, cc in lanes(OFFS[j], WIDTHS[j]):
            ux[u] = (acc_s[q, mine, cc] + rb_s[u].astype(F32) + yr[u].astype(F32)).astype(BF16)
        over_x(j).start()

    def finish(j):
        over_x(j).wait_recv()
        for u, q, cc in lanes(OFFS[j], WIDTHS[j]):
            y_ref[mine, pl.ds(u * TU, TU)] = (ux[u].astype(F32) + xr[u].astype(F32)).astype(BF16)

    sent = tuple(y_unit(i) for i in range(NR + NC))
    for u in sent:
        x_read(u, mine, 0).start()
    fence()
    for k in range(NK):
        for c in w_copies(k):
            c.start()
        if k == 0:
            fence()
            for i in range(NR):
                x_read(relay_u(i, 1 - chip), mine, 0).start()
            for u in range(NX):
                x_read(u, theirs, 1).start()
        fence()
    for j in range(ND):
        wd_copy(j).start()
    pl.semaphore_wait(barrier, 3)
    for i, u in enumerate(sent):
        x_read(u, mine, 0).wait()
        y_x(i).start()

    for kind, i, *rest in SCHEDULE:
        if kind == "y":
            on_y(i)
        elif kind == "x":
            on_x(i)
        elif kind == "s":
            own(i, *rest)
        elif kind == "o":
            other(i, *rest)
        elif kind == "t":
            term(h_o, acc_o, tb_o, OFFS[i], WIDTHS[i])
            core_o(i).start()
        elif kind == "S":
            term(h_s, acc_s, tb_s, OWN_O[i], OWN_W[i])
            core_s(i).start()
        elif kind == "e":
            send_y(i)
        elif kind == "c":
            send_x(i)
        elif kind == "f":
            finish(i)
        else:
            gather(i).start()

    for j in range(NG):
        gather(j).wait_recv()
    for i in range(NR + NC):
        y_x(i).wait_send()
    for i in range(NR):
        x_x(i, chip).wait_send()
    for m in range(NX):
        d_x(m).wait_send()
    for j in range(NT):
        core_o(j).wait_send()
        over_y(j).wait_send()
        over_x(j).wait_send()
    for j in range(NS):
        core_s(j).wait_send()
    for j in range(NG):
        gather(j).wait_send()


def mlp(x, w_gate, w_up, w_down):
    dma = pltpu.SemaphoreType.DMA
    half = pltpu.VMEM((D // TU, HALF, TU), BF16)
    return pl.pallas_call(
        kernel,
        name="mlp",
        out_shape=pltpu.VMEM((ROWS, D), BF16),
        in_specs=[pl.BlockSpec(memory_space=pl.ANY)] * 4,
        out_specs=pl.BlockSpec(memory_space=pltpu.VMEM),
        scratch_shapes=[
            pltpu.VMEM((NX, ROWS, XC), BF16),
            pltpu.VMEM((NX, ROWS, XC), BF16),
            pltpu.VMEM((NK, KC, FH), BF16),
            pltpu.VMEM((NK, KC, FH), BF16),
            pltpu.VMEM((ND, FH, DB), BF16),
            pltpu.VMEM((2, ROWS, FH), F32),
            pltpu.VMEM((2, ROWS, FH), F32),
            pltpu.VMEM((ROWS, FH), BF16),
            pltpu.VMEM((ROWS, FH), BF16),
            half, half, half, half, half, half, half, half,
            pltpu.SemaphoreType.REGULAR,
            dma((2, NX)), dma((NK,)), dma((NK,)), dma((ND,)),
            dma((NR + NC,)), dma((NR + NC,)), dma((NR,)), dma((NR,)),
            dma((NX,)), dma((NX,)),
            dma((NT,)), dma((NT,)), dma((NT,)), dma((NT,)), dma((NS,)), dma((NS,)),
            dma((NT,)), dma((NT,)), dma((NG,)), dma((NG,)),
        ],
        compiler_params=pltpu.CompilerParams(
            collective_id=0, has_side_effects=True, vmem_limit_bytes=65011712),
    )(x, w_gate, w_up, w_down)


def solution(mesh):
    return jax.shard_map(
        mlp,
        mesh=mesh,
        in_specs=(P("dp", None), P(None, "tp"), P(None, "tp"), P("tp", None)),
        out_specs=P("dp", None),
        check_vma=False,
    )
```

```python
import jax
import jax.numpy as jnp
from jax import lax
from jax.experimental import pallas as pl
from jax.experimental.pallas import tpu as pltpu
from jax.sharding import PartitionSpec as P

MESH = pl.DeviceIdType.MESH
F32 = jnp.float32
BF16 = jnp.bfloat16
ROWS = 128
HALF = ROWS // 2
D = 4096
F = 4096
FH = F // 2
KC = 512
NK = D // KC
XC = 512
NR = 3
NC = 2
NB = 256
DB = 512
TU = 128
ND = D // DB
NX = D // XC
WIDTHS = (512, 512, 512, 512, 512, 512, 512, 512)
NT = len(WIDTHS)
OFFS = tuple(sum(WIDTHS[:j]) for j in range(NT))
OWN_W = (512, 512, 1024, 1024, 1024)
NS = len(OWN_W)
OWN_O = tuple(sum(OWN_W[:j]) for j in range(NS))
OUT_W = (2048, 1024, 512, 512)
NG = len(OUT_W)
OUT_O = tuple(sum(OUT_W[:j]) for j in range(NG))

SCHEDULE = (
    ('s',0,0), ('s',0,1), ('s',1,0), ('s',1,1), ('y',0), ('s',2,0), ('s',2,1), ('y',1), ('o','y0'), ('s',3,0),
    ('s',3,1), ('y',2), ('s',4,0), ('x',0), ('o','y1'), ('y',3), ('o','y2'), ('x',1), ('o','x0'), ('y',4),
    ('o','c0'), ('x',2), ('o','x1'), ('o','c1'), ('o','x2'), ('t',0), ('t',1), ('s',4,1), ('t',2), ('s',5,0),
    ('e',0), ('s',5,1), ('s',6,0), ('e',1), ('s',6,1), ('s',7,0), ('s',7,1), ('S',0), ('e',2), ('t',3),
    ('S',1), ('t',4), ('c',0), ('e',3), ('S',2), ('c',1), ('e',4), ('t',5), ('c',2), ('t',6), ('e',5), ('S',3),
    ('c',3), ('t',7), ('f',0), ('e',6), ('S',4), ('c',4), ('e',7), ('c',5), ('f',1), ('c',6), ('f',2), ('f',3),
    ('c',7), ('g',0), ('f',4), ('f',5), ('g',1), ('f',6), ('g',2), ('f',7), ('g',3),
)


def kernel(x_hbm, wg_hbm, wu_hbm, wd_hbm, y_ref,
           xs, xo, wg, wu, wd, acc_s, acc_o, h_s, h_o,
           tb_o, rb_o, uy, yr, tb_s, rb_s, ux, xr,
           f_sem, x_sem, g_sem, u_sem, w_sem,
           yx_send, yx_recv, xx_send, xx_recv, dx_send, dx_recv,
           do_send, do_recv, uy_send, uy_recv, ds_send, ds_recv,
           ux_send, ux_recv, gy_send, gy_recv):
    grp = lax.axis_index("dp")
    tp = lax.axis_index("tp")
    core = lax.rem(tp, 2)
    chip = tp // 2
    partner = {"tp": 2 * chip + (1 - core)}
    xpeer = {"tp": 2 * (1 - chip) + core}
    ypeer = {"dp": 1 - grp}
    mine = pl.ds(pl.multiple_of(core * HALF, HALF), HALF)
    theirs = pl.ds(pl.multiple_of((1 - core) * HALF, HALF), HALF)
    units = pl.ds(pl.multiple_of(grp * FH, FH), FH)

    def fence():
        pl.semaphore_signal(f_sem, 1)
        pl.semaphore_wait(f_sem, 1)

    barrier = pltpu.get_barrier_semaphore()
    for peer in (partner, xpeer, ypeer):
        pl.semaphore_signal(barrier, inc=1, device_id=peer, device_id_type=MESH)

    def x_read(u, rows, q):
        cols = pl.ds(u * XC if isinstance(u, int) else pl.multiple_of(u * XC, XC), XC)
        return pltpu.make_async_copy(x_hbm.at[rows, cols], xs.at[u, rows], x_sem.at[q, u])


    def w_copies(k):
        rows = pl.ds(k * KC, KC)
        return (pltpu.make_async_copy(wg_hbm.at[rows, units], wg.at[k], g_sem.at[k]),
                pltpu.make_async_copy(wu_hbm.at[rows, units], wu.at[k], u_sem.at[k]))

    def wd_copy(j):
        return pltpu.make_async_copy(wd_hbm.at[units, pl.ds(j * DB, DB)], wd.at[j], w_sem.at[j])

    def push(src, dst, send, recv, peer):
        return pltpu.make_async_remote_copy(src, dst, send, recv, device_id=peer, device_id_type=MESH)

    def relay_k(i, c):
        return 2 * i + c

    def relay_u(i, c):
        return relay_k(i, c)

    def y_unit(i):
        return relay_u(i, chip) if i < NR else NR + i

    def y_x(i):
        u = y_unit(i)
        return push(xs.at[u, mine], xo.at[u, mine], yx_send.at[i], yx_recv.at[i], ypeer)

    def x_x(i, c):
        u = relay_u(i, c)
        return push(xo.at[u, mine], xo.at[u, mine], xx_send.at[i], xx_recv.at[i], xpeer)

    def d_x(m):
        u = y_unit(m) if m < NR + NC else relay_u(m - NR - NC, 1 - chip)
        return push(xo.at[u, mine], xo.at[u, mine], dx_send.at[m], dx_recv.at[m], partner)

    def on_y(i):
        y_x(i).wait_recv()
        if i < NR:
            x_x(i, chip).start()
        d_x(i).start()

    def on_x(i):
        x_x(i, 1 - chip).wait_recv()
        d_x(NR + NC + i).start()

    waited = set()

    def wait_w(*ks):
        for k in ks:
            if k not in waited:
                waited.add(k)
                for c in w_copies(k):
                    c.wait()

    def wait_wd(j):
        if ("d", j) not in waited:
            waited.add(("d", j))
            wd_copy(j).wait()

    def gate_up(xref, acc, k, lo, hi, first, h):
        lhs = xref[k]
        for n in range(lo, hi, NB):
            nn = pl.ds(n, NB)
            g = jnp.dot(lhs, wg[k, :, nn], preferred_element_type=F32)
            u = jnp.dot(lhs, wu[k, :, nn], preferred_element_type=F32)
            if not first:
                g = acc[0, :, nn] + g
                u = acc[1, :, nn] + u
            if h is None:
                acc[0, :, nn] = g
                acc[1, :, nn] = u
            else:
                h[:, nn] = (jax.nn.silu(g) * u).astype(BF16)

    def own(k, half):
        wait_w(k)
        if "x" not in waited:
            waited.add("x")
            for i in range(NR):
                x_read(relay_u(i, 1 - chip), mine, 0).wait()
            for u in range(NX):
                x_read(u, theirs, 1).wait()
        lo, hi = (0, FH) if half == 2 else (half * (FH // 2), (half + 1) * (FH // 2))
        gate_up(xs, acc_s, k, lo, hi, k == 0, h_s if k == NK - 1 else None)

    slots = [t[1] for t in SCHEDULE if t[0] == "o"]

    def other(slot):
        kind, r = slot[0], int(slot[1])
        if kind == "c":
            k, ready = 2 * NR + r, NR + r
            wait_w(k)
        else:
            wait_w(2 * r, 2 * r + 1)
            k = relay_k(r, chip if kind == "y" else 1 - chip)
            ready = r if kind == "y" else NR + NC + r
        d_x(ready).wait_recv()
        gate_up(xo, acc_o, k, 0, FH, slot == slots[0], h_o if slot == slots[-1] else None)

    def lanes(o, w):
        for p in range(o, o + w, TU):
            yield p // TU, p // FH, pl.ds(p % FH, TU)

    def term(h, acc, tb, o, w):
        for p in range(o, o + w, DB):
            wait_wd(p // DB)
        for p in range(o, o + w, min(w, DB)):
            n = min(w, DB)
            acc[p // FH, :, pl.ds(p % FH, n)] = jnp.dot(
                h[...], wd[p // DB, :, pl.ds(p % DB, n)], preferred_element_type=F32)
        for u, q, cc in lanes(o, w):
            tb[u] = acc[q, theirs, cc].astype(BF16)

    def hop(src, dst, send, recv, j, o, w, peer):
        units = pl.ds(o // TU, w // TU)
        return push(src.at[units], dst.at[units], send.at[j], recv.at[j], peer)

    def core_o(j):
        return hop(tb_o, rb_o, do_send, do_recv, j, OFFS[j], WIDTHS[j], partner)

    def core_s(j):
        return hop(tb_s, rb_s, ds_send, ds_recv, j, OWN_O[j], OWN_W[j], partner)

    def over_y(j):
        return hop(uy, yr, uy_send, uy_recv, j, OFFS[j], WIDTHS[j], ypeer)

    def over_x(j):
        return hop(ux, xr, ux_send, ux_recv, j, OFFS[j], WIDTHS[j], xpeer)

    def gather(j):
        rows = y_ref.at[mine, pl.ds(OUT_O[j], OUT_W[j])]
        return push(rows, rows, gy_send.at[j], gy_recv.at[j], partner)

    def send_y(j):
        core_o(j).wait_recv()
        for u, q, cc in lanes(OFFS[j], WIDTHS[j]):
            uy[u] = (acc_o[q, mine, cc] + rb_o[u].astype(F32)).astype(BF16)
        over_y(j).start()

    def send_x(j):
        for m in range(NS):
            if OWN_O[m] < OFFS[j] + WIDTHS[j] and OWN_O[m] + OWN_W[m] > OFFS[j] and ("s", m) not in waited:
                waited.add(("s", m))
                core_s(m).wait_recv()
        over_y(j).wait_recv()
        for u, q, cc in lanes(OFFS[j], WIDTHS[j]):
            ux[u] = (acc_s[q, mine, cc] + rb_s[u].astype(F32) + yr[u].astype(F32)).astype(BF16)
        over_x(j).start()

    def finish(j):
        over_x(j).wait_recv()
        for u, q, cc in lanes(OFFS[j], WIDTHS[j]):
            y_ref[mine, pl.ds(u * TU, TU)] = (ux[u].astype(F32) + xr[u].astype(F32)).astype(BF16)

    sent = tuple(y_unit(i) for i in range(NR + NC))
    for u in sent:
        x_read(u, mine, 0).start()
    fence()
    for k in range(NK):
        for c in w_copies(k):
            c.start()
        if k == 0:
            fence()
            for i in range(NR):
                x_read(relay_u(i, 1 - chip), mine, 0).start()
            for u in range(NX):
                x_read(u, theirs, 1).start()
        fence()
    for j in range(ND):
        wd_copy(j).start()
    pl.semaphore_wait(barrier, 3)
    for i, u in enumerate(sent):
        x_read(u, mine, 0).wait()
        y_x(i).start()

    for kind, i, *rest in SCHEDULE:
        if kind == "y":
            on_y(i)
        elif kind == "x":
            on_x(i)
        elif kind == "s":
            own(i, *rest)
        elif kind == "o":
            other(i, *rest)
        elif kind == "t":
            term(h_o, acc_o, tb_o, OFFS[i], WIDTHS[i])
            core_o(i).start()
        elif kind == "S":
            term(h_s, acc_s, tb_s, OWN_O[i], OWN_W[i])
            core_s(i).start()
        elif kind == "e":
            send_y(i)
        elif kind == "c":
            send_x(i)
        elif kind == "f":
            finish(i)
        else:
            gather(i).start()

    for j in range(NG):
        gather(j).wait_recv()
    for i in range(NR + NC):
        y_x(i).wait_send()
    for i in range(NR):
        x_x(i, chip).wait_send()
    for m in range(NX):
        d_x(m).wait_send()
    for j in range(NT):
        core_o(j).wait_send()
        over_y(j).wait_send()
        over_x(j).wait_send()
    for j in range(NS):
        core_s(j).wait_send()
    for j in range(NG):
        gather(j).wait_send()


def mlp(x, w_gate, w_up, w_down):
    dma = pltpu.SemaphoreType.DMA
    half = pltpu.VMEM((D // TU, HALF, TU), BF16)
    return pl.pallas_call(
        kernel,
        name="mlp",
        out_shape=pltpu.VMEM((ROWS, D), BF16),
        in_specs=[pl.BlockSpec(memory_space=pl.ANY)] * 4,
        out_specs=pl.BlockSpec(memory_space=pltpu.VMEM),
        scratch_shapes=[
            pltpu.VMEM((NX, ROWS, XC), BF16),
            pltpu.VMEM((NX, ROWS, XC), BF16),
            pltpu.VMEM((NK, KC, FH), BF16),
            pltpu.VMEM((NK, KC, FH), BF16),
            pltpu.VMEM((ND, FH, DB), BF16),
            pltpu.VMEM((2, ROWS, FH), F32),
            pltpu.VMEM((2, ROWS, FH), F32),
            pltpu.VMEM((ROWS, FH), BF16),
            pltpu.VMEM((ROWS, FH), BF16),
            half, half, half, half, half, half, half, half,
            pltpu.SemaphoreType.REGULAR,
            dma((2, NX)), dma((NK,)), dma((NK,)), dma((ND,)),
            dma((NR + NC,)), dma((NR + NC,)), dma((NR,)), dma((NR,)),
            dma((NX,)), dma((NX,)),
            dma((NT,)), dma((NT,)), dma((NT,)), dma((NT,)), dma((NS,)), dma((NS,)),
            dma((NT,)), dma((NT,)), dma((NG,)), dma((NG,)),
        ],
        compiler_params=pltpu.CompilerParams(
            collective_id=0, has_side_effects=True, vmem_limit_bytes=65011712),
    )(x, w_gate, w_up, w_down)


def solution(mesh):
    return jax.shard_map(
        mlp,
        mesh=mesh,
        in_specs=(P("dp", None), P(None, "tp"), P(None, "tp"), P("tp", None)),
        out_specs=P("dp", None),
        check_vma=False,
    )
```

```python
import jax
import jax.numpy as jnp
from jax import lax
from jax.experimental import pallas as pl
from jax.experimental.pallas import tpu as pltpu
from jax.sharding import PartitionSpec as P

MESH = pl.DeviceIdType.MESH
F32 = jnp.float32
BF16 = jnp.bfloat16
ROWS = 128
HALF = ROWS // 2
D = 4096
F = 4096
FH = F // 2
KC = 512
NK = D // KC
XC = 512
NR = 3
NC = 2
NB = 256
DB = 512
TU = 128
ND = D // DB
NX = D // XC
WIDTHS = (512, 512, 512, 512, 512, 512, 512, 512)
NT = len(WIDTHS)
OFFS = tuple(sum(WIDTHS[:j]) for j in range(NT))
OWN_W = (512, 512, 512, 512, 1024, 1024)
NS = len(OWN_W)
OWN_O = tuple(sum(OWN_W[:j]) for j in range(NS))
OUT_W = (1024, 1024, 1024, 512, 512)
NG = len(OUT_W)
OUT_O = tuple(sum(OUT_W[:j]) for j in range(NG))

SCHEDULE = (
    ('s',0,0), ('s',0,1), ('s',1,0), ('s',1,1), ('y',0), ('s',2,0), ('s',2,1), ('y',1), ('o','y0'), ('s',3,0),
    ('s',3,1), ('y',2), ('s',4,0), ('x',0), ('o','y1'), ('y',3), ('o','y2'), ('x',1), ('o','x0'), ('y',4),
    ('o','c0'), ('x',2), ('o','x1'), ('o','c1'), ('o','x2'), ('t',0), ('t',1), ('s',4,1), ('t',2), ('s',5,0),
    ('e',0), ('s',5,1), ('e',1), ('s',6,0), ('s',6,1), ('s',7,0), ('s',7,1), ('S',0), ('e',2), ('t',3),
    ('S',1), ('c',0), ('t',4), ('e',3), ('S',2), ('c',1), ('t',5), ('e',4), ('t',6), ('S',3), ('c',2), ('t',7),
    ('e',5), ('S',4), ('f',0), ('c',3), ('e',6), ('S',5), ('c',4), ('f',1), ('e',7), ('c',5), ('c',6), ('g',0),
    ('f',2), ('c',7), ('f',3), ('f',4), ('f',5), ('g',1), ('g',2), ('f',6), ('g',3), ('f',7), ('g',4),
)


def kernel(x_hbm, wg_hbm, wu_hbm, wd_hbm, y_ref,
           xs, xo, wg, wu, wd, acc_s, acc_o, h_s, h_o,
           tb_o, rb_o, uy, yr, tb_s, rb_s, ux, xr,
           f_sem, x_sem, g_sem, u_sem, w_sem,
           yx_send, yx_recv, xx_send, xx_recv, dx_send, dx_recv,
           do_send, do_recv, uy_send, uy_recv, ds_send, ds_recv,
           ux_send, ux_recv, gy_send, gy_recv):
    grp = lax.axis_index("dp")
    tp = lax.axis_index("tp")
    core = lax.rem(tp, 2)
    chip = tp // 2
    partner = {"tp": 2 * chip + (1 - core)}
    xpeer = {"tp": 2 * (1 - chip) + core}
    ypeer = {"dp": 1 - grp}
    mine = pl.ds(pl.multiple_of(core * HALF, HALF), HALF)
    theirs = pl.ds(pl.multiple_of((1 - core) * HALF, HALF), HALF)
    units = pl.ds(pl.multiple_of(grp * FH, FH), FH)

    def fence():
        pl.semaphore_signal(f_sem, 1)
        pl.semaphore_wait(f_sem, 1)

    barrier = pltpu.get_barrier_semaphore()
    for peer in (partner, xpeer, ypeer):
        pl.semaphore_signal(barrier, inc=1, device_id=peer, device_id_type=MESH)

    def x_read(u, rows, q):
        cols = pl.ds(u * XC if isinstance(u, int) else pl.multiple_of(u * XC, XC), XC)
        return pltpu.make_async_copy(x_hbm.at[rows, cols], xs.at[u, rows], x_sem.at[q, u])


    def w_copies(k):
        rows = pl.ds(k * KC, KC)
        return (pltpu.make_async_copy(wg_hbm.at[rows, units], wg.at[k], g_sem.at[k]),
                pltpu.make_async_copy(wu_hbm.at[rows, units], wu.at[k], u_sem.at[k]))

    def wd_copy(j):
        return pltpu.make_async_copy(wd_hbm.at[units, pl.ds(j * DB, DB)], wd.at[j], w_sem.at[j])

    def push(src, dst, send, recv, peer):
        return pltpu.make_async_remote_copy(src, dst, send, recv, device_id=peer, device_id_type=MESH)

    def relay_k(i, c):
        return 2 * i + c

    def relay_u(i, c):
        return relay_k(i, c)

    def y_unit(i):
        return relay_u(i, chip) if i < NR else NR + i

    def y_x(i):
        u = y_unit(i)
        return push(xs.at[u, mine], xo.at[u, mine], yx_send.at[i], yx_recv.at[i], ypeer)

    def x_x(i, c):
        u = relay_u(i, c)
        return push(xo.at[u, mine], xo.at[u, mine], xx_send.at[i], xx_recv.at[i], xpeer)

    def d_x(m):
        u = y_unit(m) if m < NR + NC else relay_u(m - NR - NC, 1 - chip)
        return push(xo.at[u, mine], xo.at[u, mine], dx_send.at[m], dx_recv.at[m], partner)

    def on_y(i):
        y_x(i).wait_recv()
        if i < NR:
            x_x(i, chip).start()
        d_x(i).start()

    def on_x(i):
        x_x(i, 1 - chip).wait_recv()
        d_x(NR + NC + i).start()

    waited = set()

    def wait_w(*ks):
        for k in ks:
            if k not in waited:
                waited.add(k)
                for c in w_copies(k):
                    c.wait()

    def wait_wd(j):
        if ("d", j) not in waited:
            waited.add(("d", j))
            wd_copy(j).wait()

    def gate_up(xref, acc, k, lo, hi, first, h):
        lhs = xref[k]
        for n in range(lo, hi, NB):
            nn = pl.ds(n, NB)
            g = jnp.dot(lhs, wg[k, :, nn], preferred_element_type=F32)
            u = jnp.dot(lhs, wu[k, :, nn], preferred_element_type=F32)
            if not first:
                g = acc[0, :, nn] + g
                u = acc[1, :, nn] + u
            if h is None:
                acc[0, :, nn] = g
                acc[1, :, nn] = u
            else:
                h[:, nn] = (jax.nn.silu(g) * u).astype(BF16)

    def own(k, half):
        wait_w(k)
        if "x" not in waited:
            waited.add("x")
            for i in range(NR):
                x_read(relay_u(i, 1 - chip), mine, 0).wait()
            for u in range(NX):
                x_read(u, theirs, 1).wait()
        lo, hi = (0, FH) if half == 2 else (half * (FH // 2), (half + 1) * (FH // 2))
        gate_up(xs, acc_s, k, lo, hi, k == 0, h_s if k == NK - 1 else None)

    slots = [t[1] for t in SCHEDULE if t[0] == "o"]

    def other(slot):
        kind, r = slot[0], int(slot[1])
        if kind == "c":
            k, ready = 2 * NR + r, NR + r
            wait_w(k)
        else:
            wait_w(2 * r, 2 * r + 1)
            k = relay_k(r, chip if kind == "y" else 1 - chip)
            ready = r if kind == "y" else NR + NC + r
        d_x(ready).wait_recv()
        gate_up(xo, acc_o, k, 0, FH, slot == slots[0], h_o if slot == slots[-1] else None)

    def lanes(o, w):
        for p in range(o, o + w, TU):
            yield p // TU, p // FH, pl.ds(p % FH, TU)

    def term(h, acc, tb, o, w):
        for p in range(o, o + w, DB):
            wait_wd(p // DB)
        for p in range(o, o + w, min(w, DB)):
            n = min(w, DB)
            acc[p // FH, :, pl.ds(p % FH, n)] = jnp.dot(
                h[...], wd[p // DB, :, pl.ds(p % DB, n)], preferred_element_type=F32)
        for u, q, cc in lanes(o, w):
            tb[u] = acc[q, theirs, cc].astype(BF16)

    def hop(src, dst, send, recv, j, o, w, peer):
        units = pl.ds(o // TU, w // TU)
        return push(src.at[units], dst.at[units], send.at[j], recv.at[j], peer)

    def core_o(j):
        return hop(tb_o, rb_o, do_send, do_recv, j, OFFS[j], WIDTHS[j], partner)

    def core_s(j):
        return hop(tb_s, rb_s, ds_send, ds_recv, j, OWN_O[j], OWN_W[j], partner)

    def over_y(j):
        return hop(uy, yr, uy_send, uy_recv, j, OFFS[j], WIDTHS[j], ypeer)

    def over_x(j):
        return hop(ux, xr, ux_send, ux_recv, j, OFFS[j], WIDTHS[j], xpeer)

    def gather(j):
        rows = y_ref.at[mine, pl.ds(OUT_O[j], OUT_W[j])]
        return push(rows, rows, gy_send.at[j], gy_recv.at[j], partner)

    def send_y(j):
        core_o(j).wait_recv()
        for u, q, cc in lanes(OFFS[j], WIDTHS[j]):
            uy[u] = (acc_o[q, mine, cc] + rb_o[u].astype(F32)).astype(BF16)
        over_y(j).start()

    def send_x(j):
        for m in range(NS):
            if OWN_O[m] < OFFS[j] + WIDTHS[j] and OWN_O[m] + OWN_W[m] > OFFS[j] and ("s", m) not in waited:
                waited.add(("s", m))
                core_s(m).wait_recv()
        over_y(j).wait_recv()
        for u, q, cc in lanes(OFFS[j], WIDTHS[j]):
            ux[u] = (acc_s[q, mine, cc] + rb_s[u].astype(F32) + yr[u].astype(F32)).astype(BF16)
        over_x(j).start()

    def finish(j):
        over_x(j).wait_recv()
        for u, q, cc in lanes(OFFS[j], WIDTHS[j]):
            y_ref[mine, pl.ds(u * TU, TU)] = (ux[u].astype(F32) + xr[u].astype(F32)).astype(BF16)

    sent = tuple(y_unit(i) for i in range(NR + NC))
    for u in sent:
        x_read(u, mine, 0).start()
    fence()
    for k in range(NK):
        for c in w_copies(k):
            c.start()
        if k == 0:
            fence()
            for i in range(NR):
                x_read(relay_u(i, 1 - chip), mine, 0).start()
            for u in range(NX):
                x_read(u, theirs, 1).start()
        fence()
    for j in range(ND):
        wd_copy(j).start()
    pl.semaphore_wait(barrier, 3)
    for i, u in enumerate(sent):
        x_read(u, mine, 0).wait()
        y_x(i).start()

    for kind, i, *rest in SCHEDULE:
        if kind == "y":
            on_y(i)
        elif kind == "x":
            on_x(i)
        elif kind == "s":
            own(i, *rest)
        elif kind == "o":
            other(i, *rest)
        elif kind == "t":
            term(h_o, acc_o, tb_o, OFFS[i], WIDTHS[i])
            core_o(i).start()
        elif kind == "S":
            term(h_s, acc_s, tb_s, OWN_O[i], OWN_W[i])
            core_s(i).start()
        elif kind == "e":
            send_y(i)
        elif kind == "c":
            send_x(i)
        elif kind == "f":
            finish(i)
        else:
            gather(i).start()

    for j in range(NG):
        gather(j).wait_recv()
    for i in range(NR + NC):
        y_x(i).wait_send()
    for i in range(NR):
        x_x(i, chip).wait_send()
    for m in range(NX):
        d_x(m).wait_send()
    for j in range(NT):
        core_o(j).wait_send()
        over_y(j).wait_send()
        over_x(j).wait_send()
    for j in range(NS):
        core_s(j).wait_send()
    for j in range(NG):
        gather(j).wait_send()


def mlp(x, w_gate, w_up, w_down):
    dma = pltpu.SemaphoreType.DMA
    half = pltpu.VMEM((D // TU, HALF, TU), BF16)
    return pl.pallas_call(
        kernel,
        name="mlp",
        out_shape=pltpu.VMEM((ROWS, D), BF16),
        in_specs=[pl.BlockSpec(memory_space=pl.ANY)] * 4,
        out_specs=pl.BlockSpec(memory_space=pltpu.VMEM),
        scratch_shapes=[
            pltpu.VMEM((NX, ROWS, XC), BF16),
            pltpu.VMEM((NX, ROWS, XC), BF16),
            pltpu.VMEM((NK, KC, FH), BF16),
            pltpu.VMEM((NK, KC, FH), BF16),
            pltpu.VMEM((ND, FH, DB), BF16),
            pltpu.VMEM((2, ROWS, FH), F32),
            pltpu.VMEM((2, ROWS, FH), F32),
            pltpu.VMEM((ROWS, FH), BF16),
            pltpu.VMEM((ROWS, FH), BF16),
            half, half, half, half, half, half, half, half,
            pltpu.SemaphoreType.REGULAR,
            dma((2, NX)), dma((NK,)), dma((NK,)), dma((ND,)),
            dma((NR + NC,)), dma((NR + NC,)), dma((NR,)), dma((NR,)),
            dma((NX,)), dma((NX,)),
            dma((NT,)), dma((NT,)), dma((NT,)), dma((NT,)), dma((NS,)), dma((NS,)),
            dma((NT,)), dma((NT,)), dma((NG,)), dma((NG,)),
        ],
        compiler_params=pltpu.CompilerParams(
            collective_id=0, has_side_effects=True, vmem_limit_bytes=65011712),
    )(x, w_gate, w_up, w_down)


def solution(mesh):
    return jax.shard_map(
        mlp,
        mesh=mesh,
        in_specs=(P("dp", None), P(None, "tp"), P(None, "tp"), P("tp", None)),
        out_specs=P("dp", None),
        check_vma=False,
    )
```
